32 devices in a mesh: gx: 16 (over z, y, x), gz: 2 (over core).
Axes of the slice: x: 2, y: 2, z: 4, core: 2. Of those that a mesh axis runs over, the one named last changes fastest.
Arguments:
- flow: float32 [4, 16, 512, 128], P(None, 'gz', 'gx'), may hold values from -6 to 6
- fluid: float32 [16, 512, 128], P('gz', 'gx'), may hold values from 0.2 to 5
- density: float32 [16, 512, 128], P('gz', 'gx'), may hold values from 0.35 to 0.92
- thickness: float32 [512, 128], P('gx'), may hold values from 0.5 to 4
- bed: float32 [512, 128], P('gx'), may hold values from -6 to 6
- smb: float32 [512, 128], P('gx'), may hold values from -3 to 3
- mask: int32 [512, 128], P('gx'), may hold values from 0 to 2
Outputs:
- flow_out: float32 [4, 16, 512, 128], P(None, 'gz', 'gx')
- new_thickness: float32 [512, 128], P('gx')
- overburden: float32 [16, 512, 128], P('gz', 'gx')
The draws below stay inside these ranges and needn't reach their ends.
Inputs may be any that keep to these rules, and one draw needn't show every extreme that they name: `mask`: 0 marks an ice-free column, 1 grounded ice, 2 floating ice.
All inputs are finite; a program needn't handle non-finite values.
Results may differ from the reference program's by a relative error of at most 0.00002.
Values sent between devices are 32-bit elements; how exact they have to be, the bound alone decides.
A program may use at most 64 MiB of HBM per device.

```python
import math
import jax
import jax.numpy as jnp

NY = 128
ITERS = 2
NZ = 16
NX = 512


def set_ends(values, own_key, low, largest):
    place = [jax.random.randint(jax.random.fold_in(own_key, axis), (), 0, length) for axis, length in enumerate(values.shape)]
    widest = values.shape.index(max(values.shape))
    next_to = place[:widest] + [(place[widest] + 1) % values.shape[widest]] + place[widest + 1:]
    return values.at[tuple(place)].set(low).at[tuple(next_to)].set(largest)


def level_of(key, shape, pieces, smallest, top_value):
    def one(axis_at, parts):
        heights = jax.random.uniform(jax.random.fold_in(jax.random.fold_in(key, 6), axis_at), (parts,), jnp.float32, smallest / len(pieces), top_value / len(pieces))
        return jnp.repeat(jnp.exp(heights), shape[axis_at] // parts).reshape((-1,) + (1,) * (len(shape) - axis_at - 1))

    loudness = one(*pieces[0])
    for cut in pieces[1:]:
        loudness = loudness * one(*cut)
    return loudness


def gaussian(key, dims, deviation, most, pieces=(), held_as=jnp.bfloat16):
    loudness = level_of(key, dims, pieces, -0.22, 0.18) if pieces else 1.0
    entries = jax.random.normal(key, dims, jnp.float32) * deviation * loudness
    return jnp.minimum(jnp.maximum(entries, -most), most).astype(held_as)


def setup_inputs(seed: int = 0) -> dict:
    seeds = jax.random.split(jax.random.key(seed), 8)
    flow = gaussian(seeds[0], (4, NZ, NX, NY), 1.0, 6.0, ((1, 2), (2, 16)), jnp.float32)
    fluid = jnp.clip(jnp.exp(math.log(5.0) - 3.218876 * jax.random.uniform(seeds[1], (NZ, NX, NY), jnp.float32) ** level_of(seeds[1], (NZ, NX, NY), ((0, 2), (1, 16)), -0.2, 0.2)), 0.2, 5.0)
    density = jnp.clip(0.35 + 0.570000023 * jax.random.uniform(seeds[2], (NZ, NX, NY), jnp.float32) ** level_of(seeds[2], (NZ, NX, NY), ((0, 2), (1, 16)), -0.2, 0.2), 0.35, 0.92)
    thickness = jnp.clip(jnp.exp(math.log(4.0) - 2.0794415 * jax.random.uniform(seeds[3], (NX, NY), jnp.float32) ** level_of(seeds[3], (NX, NY), ((0, 16),), -0.2, 0.2)), 0.5, 4.0)
    bed = gaussian(seeds[4], (NX, NY), 1.0, 6.0, ((0, 16),), jnp.float32)
    smb = gaussian(seeds[5], (NX, NY), 0.5, 3.0, ((0, 16),), jnp.float32)
    mask = set_ends(jax.random.randint(seeds[6], (NX, NY), 0, 3), jax.random.fold_in(seeds[6], 1), 0, 2).astype(jnp.int32)
    return {"flow": flow, "fluid": fluid, "density": density, "thickness": thickness, "bed": bed, "smb": smb, "mask": mask}


REGULAR = 0.01
FRICTION = 2.0
VELOCITY_STEP = 0.2
PRESSURE_STEP = 0.2
TIME_STEP = 0.5


def central(field, direction):
    lead = field.ndim - 3
    upper = []
    lower = []
    for number in range(field.ndim):
        extent = field.shape[number]
        if number < lead:
            upper.append(slice(None))
            lower.append(slice(None))
        elif number == lead + direction:
            upper.append(slice(2, extent))
            lower.append(slice(0, extent - 2))
        else:
            upper.append(slice(1, extent - 1))
            lower.append(slice(1, extent - 1))
    return 0.5 * (field[tuple(upper)] - field[tuple(lower)])


def stresses(padded, fluidity):
    speed_x = padded[0]
    speed_y = padded[1]
    speed_z = padded[2]
    strain_xx = central(speed_x, 1)
    strain_yy = central(speed_y, 2)
    strain_zz = central(speed_z, 0)
    strain_xy = 0.5 * (central(speed_x, 2) + central(speed_y, 1))
    strain_xz = 0.5 * (central(speed_x, 0) + central(speed_z, 1))
    strain_yz = 0.5 * (central(speed_y, 0) + central(speed_z, 2))
    second = 0.5 * (strain_xx * strain_xx + strain_yy * strain_yy + strain_zz * strain_zz)
    second = second + strain_xy * strain_xy + strain_xz * strain_xz + strain_yz * strain_yz
    viscous = 0.5 * jnp.power(fluidity, -1.0 / 3.0) * jnp.power(second + REGULAR, -1.0 / 3.0)
    stress = 2.0 * viscous[None] * jnp.stack([strain_xx, strain_yy, strain_zz, strain_xy, strain_xz, strain_yz])
    return stress, viscous, strain_xx + strain_yy + strain_zz


def momentum(stress_padded, pressure_padded):
    force_x = central(stress_padded[0], 1) + central(stress_padded[3], 2) + central(stress_padded[4], 0) - central(pressure_padded, 1)
    force_y = central(stress_padded[3], 1) + central(stress_padded[1], 2) + central(stress_padded[5], 0) - central(pressure_padded, 2)
    force_z = central(stress_padded[4], 1) + central(stress_padded[5], 2) + central(stress_padded[2], 0) - central(pressure_padded, 0)
    return force_x, force_y, force_z


def advance(state, forces, viscous, dilation, slope_x, slope_y, ice, grounded, bottom):
    force_x = forces[0] - slope_x[None] - FRICTION * grounded[None] * bottom * state[0]
    force_y = forces[1] - slope_y[None] - FRICTION * grounded[None] * bottom * state[1]
    force_z = forces[2]
    moved = jnp.stack([
        state[0] + VELOCITY_STEP * force_x / viscous,
        state[1] + VELOCITY_STEP * force_y / viscous,
        state[2] + VELOCITY_STEP * force_z / viscous,
        state[3] - PRESSURE_STEP * viscous * dilation,
    ])
    return moved * ice[None, None]


def plane_slopes(padded):
    slope_x = 0.5 * (padded[2:, 1:-1] - padded[:-2, 1:-1])
    slope_y = 0.5 * (padded[1:-1, 2:] - padded[1:-1, :-2])
    return slope_x, slope_y


def reference(flow, fluid, density, thickness, bed, smb, mask):
    surface = bed + thickness
    slope_x, slope_y = plane_slopes(jnp.pad(surface, 1))
    ice = (mask > 0).astype(jnp.float32)
    grounded = (mask == 1).astype(jnp.float32)
    bottom = (jnp.arange(NZ) == 0).astype(jnp.float32)[:, None, None]
    state = flow
    widths = ((0, 0), (1, 1), (1, 1), (1, 1))
    for sweep in range(ITERS):
        padded = jnp.pad(state, widths)
        stress, viscous, dilation = stresses(padded, fluid)
        forces = momentum(jnp.pad(stress, widths), padded[3])
        state = advance(state, forces, viscous, dilation, slope_x, slope_y, ice, grounded, bottom)
    fluxes = thickness[None] * jnp.sum(state[:2], axis=1) / NZ
    flux_padded = jnp.pad(fluxes, ((0, 0), (1, 1), (1, 1)))
    spread = 0.5 * (flux_padded[0, 2:, 1:-1] - flux_padded[0, :-2, 1:-1])
    spread = spread + 0.5 * (flux_padded[1, 1:-1, 2:] - flux_padded[1, 1:-1, :-2])
    new_thickness = thickness + TIME_STEP * (smb - spread)
    suffix = jnp.flip(jnp.cumsum(jnp.flip(density, 0), 0), 0) - density
    overburden = new_thickness[None] * (suffix + 0.5 * density) / NZ
    return state, new_thickness, overburden
```

```python
import functools

import jax
import jax.numpy as jnp
from jax import lax
from jax.experimental import pallas as pl
from jax.experimental.pallas import tpu as pltpu
from jax.sharding import PartitionSpec as P

REGULAR = 0.01
FRICTION = 2.0
STEP = 0.2
TIME_STEP = 0.5

XH = 5
ZH = 4
PAD = 16
MESH = pl.DeviceIdType.MESH


def kernel(nx, nz, nl, nxl, flow, fluid, density, thickness, bed, smb, mask,
           flow_out, new_thickness, overburden,
           S0, S1, T, V, G, M, SM, DN, A, FX, FS, FR,
           loc, send, recv, fsend, frecv):
    gx, gz = lax.axis_index("gx"), lax.axis_index("gz")
    left, right = lax.rem(gx + nx - 1, nx), lax.rem(gx + 1, nx)
    down, up = lax.rem(gz + nz - 1, nz), lax.rem(gz + 1, nz)
    has_left, has_right = gx > 0, gx < nx - 1
    has_down, has_up = gz > 0, gz < nz - 1
    ny = flow.shape[-1]
    levels_total = nl * nz
    depth, rows = S0.shape[1], S0.shape[2]
    if nz == 2:
        base = 1 + ZH * gz
        base_up, base_down = 1 + ZH, 1

        def span(h):
            return base - h * gz, nl + h
    else:
        base = base_up = base_down = 1 + ZH

        def span(h):
            return base - h, nl + 2 * h

    own = pl.ds(base, nl)
    mine = slice(PAD, PAD + nxl)
    lo, hi = PAD - 8, PAD + nxl + 8
    c, m, p = slice(lo, hi), slice(lo - 1, hi - 1), slice(lo + 1, hi + 1)
    width = hi - lo

    copies = [
        pltpu.make_async_copy(flow, S0.at[pl.ds(0, 4), own, mine], loc.at[0]),
        pltpu.make_async_copy(fluid, S0.at[4, own, mine], loc.at[1]),
        pltpu.make_async_copy(thickness, G.at[0, mine], loc.at[2]),
        pltpu.make_async_copy(bed, G.at[1, mine], loc.at[3]),
        pltpu.make_async_copy(mask, M.at[mine], loc.at[4]),
        pltpu.make_async_copy(density, DN, loc.at[5]),
        pltpu.make_async_copy(smb, SM, loc.at[6]),
    ]
    for copy in copies:
        copy.start()

    barrier = pltpu.get_barrier_semaphore()

    @pl.when(has_left)
    def _():
        pl.semaphore_signal(barrier, inc=1, device_id={"gx": left}, device_id_type=MESH)

    @pl.when(has_right)
    def _():
        pl.semaphore_signal(barrier, inc=1, device_id={"gx": right}, device_id_type=MESH)

    for off in range(1, nz):
        pl.semaphore_signal(barrier, inc=1, device_id={"gz": lax.rem(gz + off, nz)}, device_id_type=MESH)

    zrow = jnp.zeros((rows, ny), jnp.float32)
    for k in (0, depth - 1):
        for f in range(4):
            S0[f, k] = zrow
            S1[f, k] = zrow
        for f in range(3):
            T[f, k] = zrow

    def outside_x(where):
        strip = slice(PAD - 8, PAD) if where == 0 else slice(PAD + nxl, PAD + nxl + 8)
        zero = jnp.zeros((8, ny), jnp.float32)

        def one(k, _):
            for f in range(4):
                S0[f, k, strip] = zero
            S0[4, k, strip] = zero + 1.0
            return 0

        lax.fori_loop(1, depth - 1, one, 0)
        G[0, strip] = zero
        G[1, strip] = zero
        M[strip] = jnp.zeros((8, ny), jnp.int32)

    @pl.when(jnp.logical_not(has_left))
    def _():
        outside_x(0)

    @pl.when(jnp.logical_not(has_right))
    def _():
        outside_x(1)

    if nz > 2:
        def outside_z(start):
            for k in range(start, start + ZH):
                for f in range(4):
                    S0[f, k, c] = jnp.zeros((width, ny), jnp.float32)
                S0[4, k, c] = jnp.ones((width, ny), jnp.float32)

        @pl.when(jnp.logical_not(has_down))
        def _():
            outside_z(1)

        @pl.when(jnp.logical_not(has_up))
        def _():
            outside_z(1 + ZH + nl)

    def remote(src, dst, number, device):
        return pltpu.make_async_remote_copy(src_ref=src, dst_ref=dst, send_sem=send.at[number],
                                            recv_sem=recv.at[number], device_id=device, device_id_type=MESH)

    first, last = pl.ds(PAD, XH), pl.ds(PAD + nxl - XH, XH)
    from_left, from_right = pl.ds(PAD - XH, XH), pl.ds(PAD + nxl, XH)
    every = pl.ds(0, 5)
    leftward = [
        remote(S0.at[every, own, first], S0.at[every, own, from_right], 0, {"gx": left}),
        remote(G.at[:, first], G.at[:, from_right], 1, {"gx": left}),
        remote(M.at[first], M.at[from_right], 2, {"gx": left}),
    ]
    rightward = [
        remote(S0.at[every, own, last], S0.at[every, own, from_left], 3, {"gx": right}),
        remote(G.at[:, last], G.at[:, from_left], 4, {"gx": right}),
        remote(M.at[last], M.at[from_left], 5, {"gx": right}),
    ]
    top, bottom = pl.ds(base + nl - ZH, ZH), pl.ds(base, ZH)
    from_down, from_up = pl.ds(base_up - ZH, ZH), pl.ds(base_down + nl, ZH)
    pieces = (pl.ds(PAD, nxl), from_left, from_right)
    upward = [remote(S0.at[every, top, piece], S0.at[every, from_down, piece], 6 + n, {"gz": up})
              for n, piece in enumerate(pieces)]
    downward = [remote(S0.at[every, bottom, piece], S0.at[every, from_up, piece], 9 + n, {"gz": down})
                for n, piece in enumerate(pieces)]

    for n in range(5):
        copies[n].wait()
    pl.semaphore_wait(barrier, nz - 1 + jnp.where(has_left, 1, 0) + jnp.where(has_right, 1, 0))

    @pl.when(has_left)
    def _():
        for copy in leftward:
            copy.start()

    @pl.when(has_right)
    def _():
        for copy in rightward:
            copy.start()

    @pl.when(has_up)
    def _():
        upward[0].start()

    @pl.when(has_down)
    def _():
        downward[0].start()

    copies[5].wait()
    copies[6].wait()
    total = jnp.zeros((nxl, ny), jnp.float32)
    for k in reversed(range(nl)):
        cell = DN[k]
        DN[k] = total + 0.5 * cell
        total = total + cell
    FS[2, mine] = total

    def dy(f):
        axis = f.ndim - 1
        lane = lax.broadcasted_iota(jnp.int32, f.shape, axis)
        return (jnp.where(lane < ny - 1, pltpu.roll(f, ny - 1, axis), 0.0)
                - jnp.where(lane > 0, pltpu.roll(f, 1, axis), 0.0))

    def inside(start, height):
        column = gx * nxl + lax.broadcasted_iota(jnp.int32, (height, ny), 0) + (start - PAD)
        return (column >= 0) & (column < nx * nxl)

    def plan(start, height):
        c = slice(start, start + height)
        A[0, c] = 0.5 * (FX[start + 1:start + height + 1] - FX[start - 1:start + height - 1])
        A[1, c] = 0.5 * dy(FX[c])
        A[2, c] = jnp.where(inside(start, height) & (M[c] > 0), 1.0, 0.0)
        A[3, c] = jnp.where(M[c] == 1, FRICTION, 0.0)

    def level_at(k, count):
        return gz * nl + k - base + lax.broadcasted_iota(jnp.int32, (count, 1, ny), 0)

    def stress(B, k, count, start, height):
        at = pl.ds(k, count)
        c = slice(start, start + height)
        m, p = slice(start - 1, start + height - 1), slice(start + 1, start + height + 1)
        above, below = pl.ds(k + 1, count), pl.ds(k - 1, count)
        xx, vx, wx = (B[f, at, p] - B[f, at, m] for f in range(3))
        uz, vz, zz = (B[f, above, c] - B[f, below, c] for f in range(3))
        uy, yy, wy = (dy(B[f, at, c]) for f in range(3))
        xy, xz, yz = uy + vx, uz + wx, vz + wy
        twice = xx * xx + yy * yy + zz * zz
        second = 0.0625 * (twice + twice + (xy * xy + xz * xz + yz * yz))
        third = jnp.log2(S0[4, at, c] * (second + REGULAR)) * (1.0 / 3.0)
        a = jnp.exp2(-third)
        V[0, at, c] = (2.0 * STEP) * jnp.exp2(third)
        V[1, at, c] = (0.25 * STEP) * a * (xx + yy + zz)
        h = 0.25 * a
        if height == 8:
            h = jnp.where(jnp.broadcast_to(inside(start, height)[None], h.shape), h, 0.0)
        if nz > 2:
            level = level_at(k, count)
            ok = jnp.where((level >= 0) & (level < levels_total), 1.0, 0.0)
            h = jnp.where(jnp.broadcast_to(ok, h.shape) > 0.0, h, 0.0)
        g = 0.5 * h
        T[0, at, c] = g * xz
        T[1, at, c] = g * yz
        T[2, at, c] = h * zz
        T[3, at, c] = h * xx
        T[4, at, c] = g * xy
        T[5, at, c] = h * yy

    def move(B, k, count, start, height):
        at = pl.ds(k, count)
        c = slice(start, start + height)
        m, p = slice(start - 1, start + height - 1), slice(start + 1, start + height + 1)
        above, below = pl.ds(k + 1, count), pl.ds(k - 1, count)
        level = level_at(k, count)
        drag = jnp.where(level == 0, 1.0, 0.0) * A[3, c][None]
        u, v, press = B[0, at, c], B[1, at, c], B[3, at, c]
        fx = ((T[3, at, p] - T[3, at, m]) + dy(T[4, at, c]) + (T[0, above, c] - T[0, below, c])
              - 0.5 * (B[3, at, p] - B[3, at, m]) - A[0, c][None] - drag * u)
        fy = ((T[4, at, p] - T[4, at, m]) + dy(T[5, at, c]) + (T[1, above, c] - T[1, below, c])
              - 0.5 * dy(press) - A[1, c][None] - drag * v)
        fz = ((T[0, at, p] - T[0, at, m]) + dy(T[1, at, c]) + (T[2, above, c] - T[2, below, c])
              - 0.5 * (B[3, above, c] - B[3, below, c]))
        step = V[0, at, c]
        ice = jnp.broadcast_to(A[2, c][None], u.shape)
        if nz > 2:
            ice = ice * jnp.where((level >= 0) & (level < levels_total), 1.0, 0.0)
        return [jnp.where(ice > 0.0, value, 0.0) for value in (
            u + step * fx, v + step * fy, B[2, at, c] + step * fz, press - V[1, at, c])]

    def blocks(reach, most, step, areas):
        start, count = span(reach)
        pieces = -(-count // most)
        for n in range(pieces):
            one, two = count * n // pieces, count * (n + 1) // pieces
            for area in areas:
                step(start + one, two - one, *area)

    def stress_first(*at):
        stress(S0, *at)

    def stress_last(*at):
        stress(S1, *at)

    def move_first(k, count, start, height):
        for f, value in enumerate(move(S0, k, count, start, height)):
            S1[f, pl.ds(k, count), start:start + height] = value

    def move_last(k, count, start, height):
        for f, value in enumerate(move(S1, k, count, start, height)):
            flow_out[f, pl.ds(k - base, count), start:start + height] = value

    middle = [(PAD + 1, nxl - 2)]
    FX[mine] = G[1, mine] + G[0, mine]
    plan(*middle[0])
    for flag, group in ((has_down, upward), (has_up, downward)):
        @pl.when(flag)
        def _():
            group[0].wait_recv()

    blocks(3, 2, stress_first, middle)
    blocks(2, 2, move_first, middle)
    blocks(1, 2, stress_last, middle)

    @pl.when(has_left)
    def _():
        for copy in rightward:
            copy.wait_recv()

    @pl.when(has_left & has_up)
    def _():
        upward[1].start()

    @pl.when(has_left & has_down)
    def _():
        downward[1].start()

    @pl.when(has_right)
    def _():
        for copy in leftward:
            copy.wait_recv()

    @pl.when(has_right & has_up)
    def _():
        upward[2].start()

    @pl.when(has_right & has_down)
    def _():
        downward[2].start()

    blocks(0, 2, move_last, middle)

    ends = [(PAD - 4, 8), (PAD + nxl - 4, 8)]
    for start in (PAD - 8, PAD + nxl):
        strip = slice(start, start + 8)
        FX[strip] = G[1, strip] + G[0, strip]
    for area in ends:
        plan(*area)
    for flag, group in ((has_down, upward), (has_up, downward)):
        @pl.when(flag & has_left)
        def _():
            group[1].wait_recv()

        @pl.when(flag & has_right)
        def _():
            group[2].wait_recv()

    blocks(3, 6, stress_first, ends)
    blocks(2, 6, move_first, [(PAD - 5, 8), (PAD + nxl - 3, 8)])
    blocks(1, 6, stress_last, ends)
    blocks(0, 4, move_last, ends)
    sum_u, sum_v = flow_out[0, 0, c], flow_out[1, 0, c]
    for k in range(1, nl):
        sum_u = sum_u + flow_out[0, k, c]
        sum_v = sum_v + flow_out[1, k, c]
    FS[0, c] = sum_u
    FS[1, c] = sum_v

    sums = [pltpu.make_async_remote_copy(
        src_ref=FS.at[:, pl.ds(lo, width)], dst_ref=FR.at[off - 1, :, pl.ds(lo, width)],
        send_sem=fsend.at[off - 1], recv_sem=frecv.at[off - 1],
        device_id={"gz": lax.rem(gz + off, nz)}, device_id_type=MESH) for off in range(1, nz)]
    for copy in sums:
        copy.start()
    above = jnp.zeros((nxl, ny), jnp.float32)
    for off in range(1, nz):
        sums[off - 1].wait_recv()
        sum_u = sum_u + FR[off - 1, 0, c]
        sum_v = sum_v + FR[off - 1, 1, c]
        above = above + jnp.where(gz < off, 1.0, 0.0) * FR[off - 1, 2, mine]
    part = G[0, c] * (1.0 / levels_total)
    FX[c] = part * sum_u
    flux_y = dy(part * sum_v)[8:8 + nxl]
    spread = FX[PAD + 1:PAD + nxl + 1] - FX[PAD - 1:PAD + nxl - 1] + flux_y
    fresh = G[0, mine] + TIME_STEP * (SM[...] - 0.5 * spread)
    new_thickness[...] = fresh
    weight = fresh * (1.0 / levels_total)
    for k in range(nl):
        overburden[k] = weight * (above + DN[k])

    @pl.when(has_left)
    def _():
        for copy in leftward:
            copy.wait_send()

    @pl.when(has_right)
    def _():
        for copy in rightward:
            copy.wait_send()

    for flag, group in ((has_up, upward), (has_down, downward)):
        @pl.when(flag)
        def _():
            group[0].wait_send()

        @pl.when(flag & has_left)
        def _():
            group[1].wait_send()

        @pl.when(flag & has_right)
        def _():
            group[2].wait_send()

    for copy in sums:
        copy.wait_send()


def paired(nx, nl, nxl, flow, fluid, density, thickness, bed, smb, mask,
           flow_out, new_thickness, overburden,
           S0, S1, T, V, G, M, PK, RK, SM, DN, A, FX, FM, RM, FE, RE, FD, RD,
           loc, ready, send, recv):
    gx, gz = lax.axis_index("gx"), lax.axis_index("gz")
    left, right = lax.rem(gx + nx - 1, nx), lax.rem(gx + 1, nx)
    has_left, has_right = gx > 0, gx < nx - 1
    odd = lax.rem(gx, 2)
    near = gx + 1 - 2 * odd
    far = lax.rem(gx + nx - 1 + 2 * odd, nx)
    has_far = jnp.where(odd == 1, gx, nx - 1 - gx) < nx - 1
    ny = flow.shape[-1]
    levels_total = 2 * nl
    depth, rows = S0.shape[1], S0.shape[2]
    base = 1 + ZH * gz
    own = pl.ds(base, nl)
    facing = pl.ds(1 + nl - ZH + gz * (2 * ZH - nl), ZH)
    others = pl.ds(1 + gz * 2 * ZH, nl - ZH)
    across = pl.ds(1 + gz * nl, ZH)
    mine = slice(PAD, PAD + nxl)

    barrier = pltpu.get_barrier_semaphore()
    pl.semaphore_signal(barrier, inc=1, device_id={"gx": near, "gz": 0}, device_id_type=MESH)

    @pl.when(has_far)
    def _():
        pl.semaphore_signal(barrier, inc=1, device_id={"gx": far, "gz": 1}, device_id_type=MESH)

    @pl.when(gz == 1)
    def _():
        pl.semaphore_signal(barrier, inc=1, device_id={"gz": 0}, device_id_type=MESH)

    copies = [
        pltpu.make_async_copy(flow, S0.at[pl.ds(0, 4), own, mine], loc.at[0]),
        pltpu.make_async_copy(fluid, S0.at[4, own, mine], loc.at[1]),
        pltpu.make_async_copy(thickness, G.at[0, mine], loc.at[2]),
        pltpu.make_async_copy(bed, G.at[1, mine], loc.at[3]),
        pltpu.make_async_copy(mask, M, loc.at[4]),
        pltpu.make_async_copy(density, DN, loc.at[5]),
        pltpu.make_async_copy(smb, SM, loc.at[6]),
    ]
    for copy in copies:
        copy.start()

    zrow = jnp.zeros((rows, ny), jnp.float32)
    for k in (0, depth - 1):
        for f in range(4):
            S0[f, k] = zrow
            S1[f, k] = zrow
        for f in range(3):
            T[f, k] = zrow

    def outside_x(where):
        strip = slice(PAD - 8, PAD) if where == 0 else slice(PAD + nxl, PAD + nxl + 8)
        zero = jnp.zeros((8, ny), jnp.float32)

        def one(k, _):
            for f in range(4):
                S0[f, k, strip] = zero
            S0[4, k, strip] = zero + 1.0
            return 0

        lax.fori_loop(1, depth - 1, one, 0)
        G[0, strip] = zero
        G[2, strip] = zero
        FX[strip] = zero

    @pl.when(jnp.logical_not(has_left))
    def _():
        outside_x(0)

    @pl.when(jnp.logical_not(has_right))
    def _():
        outside_x(1)

    def remote(src, dst, number, device):
        return pltpu.make_async_remote_copy(src_ref=src, dst_ref=dst, send_sem=send.at[number],
                                            recv_sem=recv.at[number], device_id=device, device_id_type=MESH)

    motion, state = pl.ds(0, 3), pl.ds(3, 2)

    def halo(levels, src, dst, number, device):
        (src_uvw, src_pf), (dst_uvw, dst_pf) = src, dst
        return [remote(S0.at[motion, levels, src_uvw], S0.at[motion, levels, dst_uvw], number, device),
                remote(S0.at[state, levels, src_pf], S0.at[state, levels, dst_pf], number + 1, device)]

    first = pl.ds(PAD, XH), pl.ds(PAD, XH - 1)
    last = pl.ds(PAD + nxl - XH, XH), pl.ds(PAD + nxl - XH + 1, XH - 1)
    from_left = pl.ds(PAD - XH, XH), pl.ds(PAD - XH + 1, XH - 1)
    from_right = pl.ds(PAD + nxl, XH), pl.ds(PAD + nxl, XH - 1)

    def sideways(src, dst, side, number, device):
        early = halo(facing, src, dst, number, device)
        early.append(remote(PK.at[side], RK.at[1 - side], number + 2, device))
        return early, halo(others, src, dst, number + 3, device)

    leftward = sideways(first, from_right, 0, 0, {"gx": left})
    rightward = sideways(last, from_left, 1, 5, {"gx": right})
    partner = {"gz": 1 - gz}
    planes = remote(S0.at[pl.ds(0, 5), facing, pl.ds(PAD, nxl)], S0.at[pl.ds(0, 5), across, pl.ds(PAD, nxl)], 10, partner)

    def corner(at, number):
        (uvw, pf) = at
        return [remote(S0.at[motion, facing, uvw], S0.at[motion, across, uvw], number, partner),
                remote(S0.at[state, facing, pf], S0.at[state, across, pf], number + 1, partner)]

    corners = corner(from_left, 11), corner(from_right, 13)
    weights = remote(FD, RD, 15, partner)
    inner = remote(FM, RM, 16, partner)
    strips = [remote(FE.at[side], RE.at[side], 17 + side, partner) for side in range(2)]
    incoming = rightward, leftward
    have = (has_left, has_right)

    for n in range(5):
        copies[n].wait()
    G[2, mine] = M[...].astype(jnp.float32)
    FX[mine] = G[1, mine] + G[0, mine]
    end = PAD + nxl
    PK[0, 0:4] = FX[PAD:PAD + 4]
    PK[0, 4:7] = G[2, PAD:PAD + 3]
    PK[0, 7:8] = G[0, PAD:PAD + 1]
    PK[1, 0:4] = FX[end - 4:end]
    PK[1, 4:7] = G[2, end - 3:end]
    PK[1, 7:8] = G[0, end - 1:end]

    @pl.when(gz == 0)
    def _():
        pl.semaphore_wait(barrier, 3)
        pl.semaphore_signal(ready.at[0], inc=1, device_id=partner, device_id_type=MESH)

    @pl.when(gz == 1)
    def _():
        pl.semaphore_wait(ready.at[0], 1)

    def launch(group, flag):
        @pl.when(flag)
        def _():
            for copy in group:
                copy.start()

    launch(leftward[0], odd == 1)
    launch(rightward[0], odd == 0)
    eager = lax.rem(gx + 1, 4) < 2
    launch(leftward[1], (odd == 1) & eager)
    launch(rightward[1], (odd == 0) & eager)
    planes.start()


    def dy(f):
        axis = f.ndim - 1
        lane = lax.broadcasted_iota(jnp.int32, f.shape, axis)
        return (jnp.where(lane < ny - 1, pltpu.roll(f, ny - 1, axis), 0.0)
                - jnp.where(lane > 0, pltpu.roll(f, 1, axis), 0.0))

    def inside(start, height):
        column = gx * nxl + lax.broadcasted_iota(jnp.int32, (height, ny), 0) + (start - PAD)
        return (column >= 0) & (column < nx * nxl)

    def plan(start, height):
        c = slice(start, start + height)
        A[0, c] = 0.5 * (FX[start + 1:start + height + 1] - FX[start - 1:start + height - 1])
        A[1, c] = 0.5 * dy(FX[c])
        A[2, c] = jnp.where(inside(start, height) & (G[2, c] > 0.0), 1.0, 0.0)
        A[3, c] = jnp.where(G[2, c] == 1.0, FRICTION, 0.0)

    def level_at(k, count):
        return gz * nl + k - base + lax.broadcasted_iota(jnp.int32, (count, 1, ny), 0)

    def stress(B, k, count, start, height):
        at = pl.ds(k, count)
        c = slice(start, start + height)
        m, p = slice(start - 1, start + height - 1), slice(start + 1, start + height + 1)
        above, below = pl.ds(k + 1, count), pl.ds(k - 1, count)
        xx, vx, wx = (B[f, at, p] - B[f, at, m] for f in range(3))
        uz, vz, zz = (B[f, above, c] - B[f, below, c] for f in range(3))
        uy, yy, wy = (dy(B[f, at, c]) for f in range(3))
        xy, xz, yz = uy + vx, uz + wx, vz + wy
        twice = xx * xx + yy * yy + zz * zz
        second = 0.0625 * (twice + twice + (xy * xy + xz * xz + yz * yz))
        third = jnp.log2(S0[4, at, c] * (second + REGULAR)) * (1.0 / 3.0)
        a = jnp.exp2(-third)
        V[0, at, c] = (2.0 * STEP) * jnp.exp2(third)
        V[1, at, c] = (0.25 * STEP) * a * (xx + yy + zz)
        h = 0.25 * a
        if height == 8:
            h = jnp.where(jnp.broadcast_to(inside(start, height)[None], h.shape), h, 0.0)
        g = 0.5 * h
        T[0, at, c] = g * xz
        T[1, at, c] = g * yz
        T[2, at, c] = h * zz
        T[3, at, c] = h * xx
        T[4, at, c] = g * xy
        T[5, at, c] = h * yy

    def move(B, k, count, start, height):
        at = pl.ds(k, count)
        c = slice(start, start + height)
        m, p = slice(start - 1, start + height - 1), slice(start + 1, start + height + 1)
        above, below = pl.ds(k + 1, count), pl.ds(k - 1, count)
        drag = jnp.where(level_at(k, count) == 0, 1.0, 0.0) * A[3, c][None]
        u, v, press = B[0, at, c], B[1, at, c], B[3, at, c]
        fx = ((T[3, at, p] - T[3, at, m]) + dy(T[4, at, c]) + (T[0, above, c] - T[0, below, c])
              - 0.5 * (B[3, at, p] - B[3, at, m]) - A[0, c][None] - drag * u)
        fy = ((T[4, at, p] - T[4, at, m]) + dy(T[5, at, c]) + (T[1, above, c] - T[1, below, c])
              - 0.5 * dy(press) - A[1, c][None] - drag * v)
        fz = ((T[0, at, p] - T[0, at, m]) + dy(T[1, at, c]) + (T[2, above, c] - T[2, below, c])
              - 0.5 * (B[3, above, c] - B[3, below, c]))
        step = V[0, at, c]
        ice = jnp.broadcast_to(A[2, c][None], u.shape)
        return [jnp.where(ice > 0.0, value, 0.0) for value in (
            u + step * fx, v + step * fy, B[2, at, c] + step * fz, press - V[1, at, c])]

    def blocks(start, count, most, step, area):
        pieces = -(-count // most)
        for n in range(pieces):
            one, two = count * n // pieces, count * (n + 1) // pieces
            step(start + one, two - one, *area)

    def apart(reach, most, step, area):
        blocks(1 + gz * (2 * ZH - reach), nl - ZH + reach, most, step, area)

    def facing_part(reach, most, step, area):
        low, high = 1 + nl - ZH + reach, 1 + ZH - reach
        blocks(low + gz * (high - low), ZH, most, step, area)

    def reached(reach, most, step, area):
        low = 1 + nl - reach
        blocks(low + gz * (1 + ZH - reach - low), 2 * (ZH - 4 + reach), most, step, area)

    def rest(reach, most, step, area):
        count = nl - reach
        blocks(1 + gz * (ZH + nl - count), count, most, step, area)

    def stress_first(*at):
        stress(S0, *at)

    def stress_last(*at):
        stress(S1, *at)

    def move_first(k, count, start, height):
        for f, value in enumerate(move(S0, k, count, start, height)):
            S1[f, pl.ds(k, count), start:start + height] = value

    def move_last(k, count, start, height):
        for f, value in enumerate(move(S1, k, count, start, height)):
            flow_out[f, pl.ds(k - base, count), start:start + height] = value

    middle = (PAD + 1, nxl - 2)
    plan(*middle)
    apart(3, 2, stress_first, middle)

    copies[5].wait()
    copies[6].wait()
    total = jnp.zeros((nxl, ny), jnp.float32)
    for k in reversed(range(nl)):
        cell = DN[k]
        DN[k] = total + 0.5 * cell
        total = total + cell
    FS[2, mine] = total

    def dy(f):
        axis = f.ndim - 1
        lane = lax.broadcasted_iota(jnp.int32, f.shape, axis)
        return (jnp.where(lane < ny - 1, pltpu.roll(f, ny - 1, axis), 0.0)
                - jnp.where(lane > 0, pltpu.roll(f, 1, axis), 0.0))

    def inside(start, height):
        column = gx * nxl + lax.broadcasted_iota(jnp.int32, (height, ny), 0) + (start - PAD)
        return (column >= 0) & (column < nx * nxl)

    def plan(start, height):
        c = slice(start, start + height)
        A[0, c] = 0.5 * (FX[start + 1:start + height + 1] - FX[start - 1:start + height - 1])
        A[1, c] = 0.5 * dy(FX[c])
        A[2, c] = jnp.where(inside(start, height) & (M[c] > 0), 1.0, 0.0)
        A[3, c] = jnp.where(M[c] == 1, FRICTION, 0.0)

    def level_at(k, count):
        return gz * nl + k - base + lax.broadcasted_iota(jnp.int32, (count, 1, ny), 0)

    def stress(B, k, count, start, height):
        at = pl.ds(k, count)
        c = slice(start, start + height)
        m, p = slice(start - 1, start + height - 1), slice(start + 1, start + height + 1)
        above, below = pl.ds(k + 1, count), pl.ds(k - 1, count)
        xx, vx, wx = (B[f, at, p] - B[f, at, m] for f in range(3))
        uz, vz, zz = (B[f, above, c] - B[f, below, c] for f in range(3))
        uy, yy, wy = (dy(B[f, at, c]) for f in range(3))
        xy, xz, yz = uy + vx, uz + wx, vz + wy
        twice = xx * xx + yy * yy + zz * zz
        second = 0.0625 * (twice + twice + (xy * xy + xz * xz + yz * yz))
        third = jnp.log2(S0[4, at, c] * (second + REGULAR)) * (1.0 / 3.0)
        a = jnp.exp2(-third)
        V[0, at, c] = (2.0 * STEP) * jnp.exp2(third)
        V[1, at, c] = (0.25 * STEP) * a * (xx + yy + zz)
        h = 0.25 * a
        if height == 8:
            h = jnp.where(jnp.broadcast_to(inside(start, height)[None], h.shape), h, 0.0)
        if nz > 2:
            level = level_at(k, count)
            ok = jnp.where((level >= 0) & (level < levels_total), 1.0, 0.0)
            h = jnp.where(jnp.broadcast_to(ok, h.shape) > 0.0, h, 0.0)
        g = 0.5 * h
        T[0, at, c] = g * xz
        T[1, at, c] = g * yz
        T[2, at, c] = h * zz
        T[3, at, c] = h * xx
        T[4, at, c] = g * xy
        T[5, at, c] = h * yy

    def move(B, k, count, start, height):
        at = pl.ds(k, count)
        c = slice(start, start + height)
        m, p = slice(start - 1, start + height - 1), slice(start + 1, start + height + 1)
        above, below = pl.ds(k + 1, count), pl.ds(k - 1, count)
        level = level_at(k, count)
        drag = jnp.where(level == 0, 1.0, 0.0) * A[3, c][None]
        u, v, press = B[0, at, c], B[1, at, c], B[3, at, c]
        fx = ((T[3, at, p] - T[3, at, m]) + dy(T[4, at, c]) + (T[0, above, c] - T[0, below, c])
              - 0.5 * (B[3, at, p] - B[3, at, m]) - A[0, c][None] - drag * u)
        fy = ((T[4, at, p] - T[4, at, m]) + dy(T[5, at, c]) + (T[1, above, c] - T[1, below, c])
              - 0.5 * dy(press) - A[1, c][None] - drag * v)
        fz = ((T[0, at, p] - T[0, at, m]) + dy(T[1, at, c]) + (T[2, above, c] - T[2, below, c])
              - 0.5 * (B[3, above, c] - B[3, below, c]))
        step = V[0, at, c]
        ice = jnp.broadcast_to(A[2, c][None], u.shape)
        if nz > 2:
            ice = ice * jnp.where((level >= 0) & (level < levels_total), 1.0, 0.0)
        return [jnp.where(ice > 0.0, value, 0.0) for value in (
            u + step * fx, v + step * fy, B[2, at, c] + step * fz, press - V[1, at, c])]

    def blocks(reach, most, step, areas):
        start, count = span(reach)
        pieces = -(-count // most)
        for n in range(pieces):
            one, two = count * n // pieces, count * (n + 1) // pieces
            for area in areas:
                step(start + one, two - one, *area)

    def stress_first(*at):
        stress(S0, *at)

    def stress_last(*at):
        stress(S1, *at)

    def move_first(k, count, start, height):
        for f, value in enumerate(move(S0, k, count, start, height)):
            S1[f, pl.ds(k, count), start:start + height] = value

    def move_last(k, count, start, height):
        for f, value in enumerate(move(S1, k, count, start, height)):
            flow_out[f, pl.ds(k - base, count), start:start + height] = value

    middle = [(PAD + 1, nxl - 2)]
    FX[mine] = G[1, mine] + G[0, mine]
    plan(*middle[0])
    for flag, group in ((has_down, upward), (has_up, downward)):
        @pl.when(flag)
        def _():
            group[0].wait_recv()

    blocks(3, 2, stress_first, middle)
    blocks(2, 2, move_first, middle)
    blocks(1, 2, stress_last, middle)

    @pl.when(has_left)
    def _():
        for copy in rightward:
            copy.wait_recv()

    @pl.when(has_left & has_up)
    def _():
        upward[1].start()

    @pl.when(has_left & has_down)
    def _():
        downward[1].start()

    @pl.when(has_right)
    def _():
        for copy in leftward:
            copy.wait_recv()

    @pl.when(has_right & has_up)
    def _():
        upward[2].start()

    @pl.when(has_right & has_down)
    def _():
        downward[2].start()

    blocks(0, 2, move_last, middle)

    ends = [(PAD - 4, 8), (PAD + nxl - 4, 8)]
    for start in (PAD - 8, PAD + nxl):
        strip = slice(start, start + 8)
        FX[strip] = G[1, strip] + G[0, strip]
    for area in ends:
        plan(*area)
    for flag, group in ((has_down, upward), (has_up, downward)):
        @pl.when(flag & has_left)
        def _():
            group[1].wait_recv()

        @pl.when(flag & has_right)
        def _():
            group[2].wait_recv()

    blocks(3, 6, stress_first, ends)
    blocks(2, 6, move_first, [(PAD - 5, 8), (PAD + nxl - 3, 8)])
    blocks(1, 6, stress_last, ends)
    blocks(0, 4, move_last, ends)
    sum_u, sum_v = flow_out[0, 0, c], flow_out[1, 0, c]
    for k in range(1, nl):
        sum_u = sum_u + flow_out[0, k, c]
        sum_v = sum_v + flow_out[1, k, c]
    FS[0, c] = sum_u
    FS[1, c] = sum_v

    sums = [pltpu.make_async_remote_copy(
        src_ref=FS.at[:, pl.ds(lo, width)], dst_ref=FR.at[off - 1, :, pl.ds(lo, width)],
        send_sem=fsend.at[off - 1], recv_sem=frecv.at[off - 1],
        device_id={"gz": lax.rem(gz + off, nz)}, device_id_type=MESH) for off in range(1, nz)]
    for copy in sums:
        copy.start()
    above = jnp.zeros((nxl, ny), jnp.float32)
    for off in range(1, nz):
        sums[off - 1].wait_recv()
        sum_u = sum_u + FR[off - 1, 0, c]
        sum_v = sum_v + FR[off - 1, 1, c]
        above = above + jnp.where(gz < off, 1.0, 0.0) * FR[off - 1, 2, mine]
    part = G[0, c] * (1.0 / levels_total)
    FX[c] = part * sum_u
    flux_y = dy(part * sum_v)[8:8 + nxl]
    spread = FX[PAD + 1:PAD + nxl + 1] - FX[PAD - 1:PAD + nxl - 1] + flux_y
    fresh = G[0, mine] + TIME_STEP * (SM[...] - 0.5 * spread)
    new_thickness[...] = fresh
    weight = fresh * (1.0 / levels_total)
    for k in range(nl):
        overburden[k] = weight * (above + DN[k])

    @pl.when(has_left)
    def _():
        for copy in leftward:
            copy.wait_send()

    @pl.when(has_right)
    def _():
        for copy in rightward:
            copy.wait_send()

    for flag, group in ((has_up, upward), (has_down, downward)):
        @pl.when(flag)
        def _():
            group[0].wait_send()

        @pl.when(flag & has_left)
        def _():
            group[1].wait_send()

        @pl.when(flag & has_right)
        def _():
            group[2].wait_send()

    for copy in sums:
        copy.wait_send()


def paired(nx, nl, nxl, flow, fluid, density, thickness, bed, smb, mask,
           flow_out, new_thickness, overburden,
           S0, S1, T, V, G, M, PK, RK, SM, DN, A, FX, FM, RM, FE, RE, FD, RD,
           loc, ready, send, recv):
    gx, gz = lax.axis_index("gx"), lax.axis_index("gz")
    left, right = lax.rem(gx + nx - 1, nx), lax.rem(gx + 1, nx)
    has_left, has_right = gx > 0, gx < nx - 1
    odd = lax.rem(gx, 2)
    near = gx + 1 - 2 * odd
    far = lax.rem(gx + nx - 1 + 2 * odd, nx)
    has_far = jnp.where(odd == 1, gx, nx - 1 - gx) < nx - 1
    ny = flow.shape[-1]
    levels_total = 2 * nl
    depth, rows = S0.shape[1], S0.shape[2]
    base = 1 + ZH * gz
    own = pl.ds(base, nl)
    facing = pl.ds(1 + nl - ZH + gz * (2 * ZH - nl), ZH)
    others = pl.ds(1 + gz * 2 * ZH, nl - ZH)
    across = pl.ds(1 + gz * nl, ZH)
    mine = slice(PAD, PAD + nxl)

    barrier = pltpu.get_barrier_semaphore()
    pl.semaphore_signal(barrier, inc=1, device_id={"gx": near, "gz": 0}, device_id_type=MESH)

    @pl.when(has_far)
    def _():
        pl.semaphore_signal(barrier, inc=1, device_id={"gx": far, "gz": 1}, device_id_type=MESH)

    @pl.when(gz == 1)
    def _():
        pl.semaphore_signal(barrier, inc=1, device_id={"gz": 0}, device_id_type=MESH)

    copies = [
        pltpu.make_async_copy(flow, S0.at[pl.ds(0, 4), own, mine], loc.at[0]),
        pltpu.make_async_copy(fluid, S0.at[4, own, mine], loc.at[1]),
        pltpu.make_async_copy(thickness, G.at[0, mine], loc.at[2]),
        pltpu.make_async_copy(bed, G.at[1, mine], loc.at[3]),
        pltpu.make_async_copy(mask, M, loc.at[4]),
        pltpu.make_async_copy(density, DN, loc.at[5]),
        pltpu.make_async_copy(smb, SM, loc.at[6]),
    ]
    for copy in copies:
        copy.start()

    zrow = jnp.zeros((rows, ny), jnp.float32)
    for k in (0, depth - 1):
        for f in range(4):
            S0[f, k] = zrow
            S1[f, k] = zrow
        for f in range(3):
            T[f, k] = zrow

    def outside_x(where):
        strip = slice(PAD - 8, PAD) if where == 0 else slice(PAD + nxl, PAD + nxl + 8)
        zero = jnp.zeros((8, ny), jnp.float32)

        def one(k, _):
            for f in range(4):
                S0[f, k, strip] = zero
            S0[4, k, strip] = zero + 1.0
            return 0

        lax.fori_loop(1, depth - 1, one, 0)
        G[0, strip] = zero
        G[2, strip] = zero
        FX[strip] = zero

    @pl.when(jnp.logical_not(has_left))
    def _():
        outside_x(0)

    @pl.when(jnp.logical_not(has_right))
    def _():
        outside_x(1)

    def remote(src, dst, number, device):
        return pltpu.make_async_remote_copy(src_ref=src, dst_ref=dst, send_sem=send.at[number],
                                            recv_sem=recv.at[number], device_id=device, device_id_type=MESH)

    motion, state = pl.ds(0, 3), pl.ds(3, 2)

    def halo(levels, src, dst, number, device):
        (src_uvw, src_pf), (dst_uvw, dst_pf) = src, dst
        return [remote(S0.at[motion, levels, src_uvw], S0.at[motion, levels, dst_uvw], number, device),
                remote(S0.at[state, levels, src_pf], S0.at[state, levels, dst_pf], number + 1, device)]

    first = pl.ds(PAD, XH), pl.ds(PAD, XH - 1)
    last = pl.ds(PAD + nxl - XH, XH), pl.ds(PAD + nxl - XH + 1, XH - 1)
    from_left = pl.ds(PAD - XH, XH), pl.ds(PAD - XH + 1, XH - 1)
    from_right = pl.ds(PAD + nxl, XH), pl.ds(PAD + nxl, XH - 1)

    def sideways(src, dst, side, number, device):
        early = halo(facing, src, dst, number, device)
        early.append(remote(PK.at[side], RK.at[1 - side], number + 2, device))
        return early, halo(others, src, dst, number + 3, device)

    leftward = sideways(first, from_right, 0, 0, {"gx": left})
    rightward = sideways(last, from_left, 1, 5, {"gx": right})
    partner = {"gz": 1 - gz}
    planes = remote(S0.at[pl.ds(0, 5), facing, pl.ds(PAD, nxl)], S0.at[pl.ds(0, 5), across, pl.ds(PAD, nxl)], 10, partner)

    def corner(at, number):
        (uvw, pf) = at
        return [remote(S0.at[motion, facing, uvw], S0.at[motion, across, uvw], number, partner),
                remote(S0.at[state, facing, pf], S0.at[state, across, pf], number + 1, partner)]

    corners = corner(from_left, 11), corner(from_right, 13)
    weights = remote(FD, RD, 15, partner)
    inner = remote(FM, RM, 16, partner)
    strips = [remote(FE.at[side], RE.at[side], 17 + side, partner) for side in range(2)]
    incoming = rightward, leftward
    have = (has_left, has_right)

    for n in range(5):
        copies[n].wait()
    G[2, mine] = M[...].astype(jnp.float32)
    FX[mine] = G[1, mine] + G[0, mine]
    end = PAD + nxl
    PK[0, 0:4] = FX[PAD:PAD + 4]
    PK[0, 4:7] = G[2, PAD:PAD + 3]
    PK[0, 7:8] = G[0, PAD:PAD + 1]
    PK[1, 0:4] = FX[end - 4:end]
    PK[1, 4:7] = G[2, end - 3:end]
    PK[1, 7:8] = G[0, end - 1:end]

    @pl.when(gz == 0)
    def _():
        pl.semaphore_wait(barrier, 3)
        pl.semaphore_signal(ready.at[0], inc=1, device_id=partner, device_id_type=MESH)

    @pl.when(gz == 1)
    def _():
        pl.semaphore_wait(ready.at[0], 1)

    def launch(group, flag):
        @pl.when(flag)
        def _():
            for copy in group:
                copy.start()

    launch(leftward[0], odd == 1)
    launch(rightward[0], odd == 0)
    eager = lax.rem(gx + 1, 4) < 2
    launch(leftward[1], (odd == 1) & eager)
    launch(rightward[1], (odd == 0) & eager)
    planes.start()

    def dy(f):
        axis = f.ndim - 1
        lane = lax.broadcasted_iota(jnp.int32, f.shape, axis)
        return (jnp.where(lane < ny - 1, pltpu.roll(f, ny - 1, axis), 0.0)
                - jnp.where(lane > 0, pltpu.roll(f, 1, axis), 0.0))

    def inside(start, height):
        column = gx * nxl + lax.broadcasted_iota(jnp.int32, (height, ny), 0) + (start - PAD)
        return (column >= 0) & (column < nx * nxl)

    def plan(start, height):
        c = slice(start, start + height)
        A[0, c] = 0.5 * (FX[start + 1:start + height + 1] - FX[start - 1:start + height - 1])
        A[1, c] = 0.5 * dy(FX[c])
        A[2, c] = jnp.where(inside(start, height) & (G[2, c] > 0.0), 1.0, 0.0)
        A[3, c] = jnp.where(G[2, c] == 1.0, FRICTION, 0.0)

    def level_at(k, count):
        return gz * nl + k - base + lax.broadcasted_iota(jnp.int32, (count, 1, ny), 0)

    def stress(B, k, count, start, height):
        at = pl.ds(k, count)
        c = slice(start, start + height)
        m, p = slice(start - 1, start + height - 1), slice(start + 1, start + height + 1)
        above, below = pl.ds(k + 1, count), pl.ds(k - 1, count)
        xx, vx, wx = (B[f, at, p] - B[f, at, m] for f in range(3))
        uz, vz, zz = (B[f, above, c] - B[f, below, c] for f in range(3))
        uy, yy, wy = (dy(B[f, at, c]) for f in range(3))
        xy, xz, yz = uy + vx, uz + wx, vz + wy
        twice = xx * xx + yy * yy + zz * zz
        second = 0.0625 * (twice + twice + (xy * xy + xz * xz + yz * yz))
        third = jnp.log2(S0[4, at, c] * (second + REGULAR)) * (1.0 / 3.0)
        a = jnp.exp2(-third)
        V[0, at, c] = (2.0 * STEP) * jnp.exp2(third)
        V[1, at, c] = (0.25 * STEP) * a * (xx + yy + zz)
        h = 0.25 * a
        if height == 8:
            h = jnp.where(jnp.broadcast_to(inside(start, height)[None], h.shape), h, 0.0)
        g = 0.5 * h
        T[0, at, c] = g * xz
        T[1, at, c] = g * yz
        T[2, at, c] = h * zz
        T[3, at, c] = h * xx
        T[4, at, c] = g * xy
        T[5, at, c] = h * yy

    def move(B, k, count, start, height):
        at = pl.ds(k, count)
        c = slice(start, start + height)
        m, p = slice(start - 1, start + height - 1), slice(start + 1, start + height + 1)
        above, below = pl.ds(k + 1, count), pl.ds(k - 1, count)
        drag = jnp.where(level_at(k, count) == 0, 1.0, 0.0) * A[3, c][None]
        u, v, press = B[0, at, c], B[1, at, c], B[3, at, c]
        fx = ((T[3, at, p] - T[3, at, m]) + dy(T[4, at, c]) + (T[0, above, c] - T[0, below, c])
              - 0.5 * (B[3, at, p] - B[3, at, m]) - A[0, c][None] - drag * u)
        fy = ((T[4, at, p] - T[4, at, m]) + dy(T[5, at, c]) + (T[1, above, c] - T[1, below, c])
              - 0.5 * dy(press) - A[1, c][None] - drag * v)
        fz = ((T[0, at, p] - T[0, at, m]) + dy(T[1, at, c]) + (T[2, above, c] - T[2, below, c])
              - 0.5 * (B[3, above, c] - B[3, below, c]))
        step = V[0, at, c]
        ice = jnp.broadcast_to(A[2, c][None], u.shape)
        return [jnp.where(ice > 0.0, value, 0.0) for value in (
            u + step * fx, v + step * fy, B[2, at, c] + step * fz, press - V[1, at, c])]

    def blocks(start, count, most, step, area):
        pieces = -(-count // most)
        for n in range(pieces):
            one, two = count * n // pieces, count * (n + 1) // pieces
            step(start + one, two - one, *area)

    def apart(reach, most, step, area):
        blocks(1 + gz * (2 * ZH - reach), nl - ZH + reach, most, step, area)

    def facing_part(reach, most, step, area):
        low, high = 1 + nl - ZH + reach, 1 + ZH - reach
        blocks(low + gz * (high - low), ZH, most, step, area)

    def reached(reach, most, step, area):
        low = 1 + nl - reach
        blocks(low + gz * (1 + ZH - reach - low), 2 * (ZH - 4 + reach), most, step, area)

    def rest(reach, most, step, area):
        count = nl - reach
        blocks(1 + gz * (ZH + nl - count), count, most, step, area)

    def stress_first(*at):
        stress(S0, *at)

    def stress_last(*at):
        stress(S1, *at)

    def move_first(k, count, start, height):
        for f, value in enumerate(move(S0, k, count, start, height)):
            S1[f, pl.ds(k, count), start:start + height] = value

    def move_last(k, count, start, height):
        for f, value in enumerate(move(S1, k, count, start, height)):
            flow_out[f, pl.ds(k - base, count), start:start + height] = value

    middle = (PAD + 1, nxl - 2)
    plan(*middle)
    apart(3, 2, stress_first, middle)

    @pl.when(has_far & (gz == 1))
    def _():
        pl.semaphore_wait(barrier, 2)
        pl.semaphore_signal(ready.at[1], inc=1, device_id=partner, device_id_type=MESH)

    @pl.when(has_far & (gz == 0))
    def _():
        pl.semaphore_wait(ready.at[1], 1)

    launch(rightward[0], (odd == 1) & has_right)
    launch(leftward[0], (odd == 0) & has_left)
    launch(leftward[1], (odd == 1) & jnp.logical_not(eager))
    launch(rightward[1], (odd == 0) & jnp.logical_not(eager))
    launch(rightward[1], (odd == 1) & has_right)
    launch(leftward[1], (odd == 0) & has_left)

    copies[5].wait()
    copies[6].wait()
    total = jnp.zeros((nxl, ny), jnp.float32)
    for k in reversed(range(nl)):
        cell = DN[k]
        DN[k] = total + 0.5 * cell
        total = total + cell
    FD[...] = total
    weights.start()

    apart(2, 2, move_first, middle)
    apart(1, 2, stress_last, middle)
    apart(0, 2, move_last, middle)
    planes.wait_recv()
    facing_part(3, 2, stress_first, middle)

    def forward(side):
        @pl.when(have[side])
        def _():
            for copy in incoming[side][0][:2]:
                copy.wait_recv()
            for copy in corners[side]:
                copy.start()

    crossed = (lax.rem(gx, 4) == 2) & (gx > 2)
    left_leads = (gx == 0) | (((odd == 1) | crossed) & has_right)

    def by_arrival(step):
        @pl.when(left_leads)
        def _():
            step(0, 1)

        @pl.when(jnp.logical_not(left_leads))
        def _():
            step(1, 0)

    facing_part(2, 2, move_first, middle)
    facing_part(1, 2, stress_last, middle)
    facing_part(0, 2, move_last, middle)

    by_arrival(lambda lead, other: forward(lead))

    def depth_sum(f, c):
        value = flow_out[f, 0, c]
        for k in range(1, nl):
            value = value + flow_out[f, k, c]
        return value

    for f in range(2):
        FM[f] = depth_sum(f, mine)
    inner.start()

    edges = [((PAD - 4, 8), (PAD - 5, 8)), ((PAD + nxl - 4, 8), (PAD + nxl - 3, 8))]

    def approach(side):
        area, shifted = edges[side]

        @pl.when(have[side])
        def _():
            incoming[side][0][2].wait_recv()
            at = PAD if side == 0 else end
            for row in range(4):
                to = at - 4 + row if side == 0 else at + row
                FX[to:to + 1] = RK[side, row:row + 1]
            for row in range(3):
                to = at - 3 + row if side == 0 else at + row
                G[2, to:to + 1] = RK[side, 4 + row:5 + row]
            to = at - 1 if side == 0 else at
            G[0, to:to + 1] = RK[side, 7:8]
            for copy in corners[side]:
                copy.wait_recv()

        plan(*area)
        reached(3, 3, stress_first, area)
        reached(2, 4, move_first, shifted)
        reached(1, 4, stress_last, area)

    def finish(side):
        area, shifted = edges[side]

        @pl.when(have[side])
        def _():
            for copy in incoming[side][1]:
                copy.wait_recv()

        rest(3, 5, stress_first, area)
        rest(2, 6, move_first, shifted)
        rest(1, 4, stress_last, area)
        rest(0, 4, move_last, area)
        wide = slice(PAD - 8, PAD + 8) if side == 0 else slice(PAD + nxl - 8, PAD + nxl + 8)
        for f in range(2):
            FE[side, f] = depth_sum(f, wide)
        strips[side].start()

    def both(lead, other):
        forward(other)
        approach(lead)
        finish(lead)
        approach(other)
        finish(other)

    by_arrival(both)

    def settle(start, height, sum_v):
        c = slice(start, start + height)
        o = slice(start - PAD, start - PAD + height)
        flux_y = dy(G[0, c] * (1.0 / levels_total) * sum_v)
        spread = FX[start + 1:start + height + 1] - FX[start - 1:start + height - 1] + flux_y
        fresh = G[0, c] + TIME_STEP * (SM[o] - 0.5 * spread)
        new_thickness[o] = fresh
        weight = fresh * (1.0 / levels_total)
        above = jnp.where(gz == 0, 1.0, 0.0) * RD[o]
        for k in range(nl):
            overburden[k, o] = weight * (above + DN[k, o])

    weights.wait_recv()
    inner.wait_recv()
    FX[mine] = G[0, mine] * (1.0 / levels_total) * (FM[0] + RM[0])
    settle(PAD + 8, nxl - 16, FM[1, 8:nxl - 8] + RM[1, 8:nxl - 8])
    for side in range(2):
        strips[side].wait_recv()
        begin = PAD - 8 if side == 0 else PAD + nxl - 8
        wide = slice(begin, begin + 16)
        FX[wide] = G[0, wide] * (1.0 / levels_total) * (FE[side, 0] + RE[side, 0])
        inward = slice(8, 16) if side == 0 else slice(0, 8)
        settle(PAD if side == 0 else PAD + nxl - 8, 8, FE[side, 1, inward] + RE[side, 1, inward])

    for side, group in ((0, leftward), (1, rightward)):
        @pl.when(have[side])
        def _():
            for copy in (*group[0], *group[1], *corners[side]):
                copy.wait_send()

    for copy in (planes, weights, inner, *strips):
        copy.wait_send()


def write(nxl, held, fresh, weight, flow_out, new_thickness, overburden, done):
    copies = [
        pltpu.make_async_copy(held.at[:, :, pl.ds(PAD, nxl)], flow_out, done.at[0]),
        pltpu.make_async_copy(fresh, new_thickness, done.at[1]),
        pltpu.make_async_copy(weight, overburden, done.at[2]),
    ]
    for copy in copies:
        copy.start()
    for copy in copies:
        copy.wait()


def solution(mesh):
    nx, nz = mesh.shape["gx"], mesh.shape["gz"]

    def body(flow, fluid, density, thickness, bed, smb, mask):
        nl, nxl, ny = fluid.shape
        depth = nl + 2 + (ZH if nz == 2 else 2 * ZH)
        rows = nxl + 2 * PAD
        f32 = jnp.float32
        vmem = pl.BlockSpec(memory_space=pltpu.VMEM)
        block = [pltpu.VMEM((n, depth, rows, ny), f32) for n in (5, 4, 6, 2)]
        if nz == 2 and nx % 2 == 0 and nl > ZH and nxl >= 24:
            body_of = functools.partial(paired, nx, nl, nxl)
            scratch = block + [
                pltpu.VMEM((3, rows, ny), f32),
                pltpu.VMEM((nxl, ny), jnp.int32),
                pltpu.VMEM((2, 8, ny), f32),
                pltpu.VMEM((2, 8, ny), f32),
                pltpu.VMEM((nxl, ny), f32),
                pltpu.VMEM((nl, nxl, ny), f32),
                pltpu.VMEM((4, rows, ny), f32),
                pltpu.VMEM((rows, ny), f32),
                pltpu.VMEM((2, nxl, ny), f32),
                pltpu.VMEM((2, nxl, ny), f32),
                pltpu.VMEM((2, 2, 16, ny), f32),
                pltpu.VMEM((2, 2, 16, ny), f32),
                pltpu.VMEM((nxl, ny), f32),
                pltpu.VMEM((nxl, ny), f32),
                pltpu.SemaphoreType.DMA((7,)),
                pltpu.SemaphoreType.REGULAR((2,)),
                pltpu.SemaphoreType.DMA((19,)),
                pltpu.SemaphoreType.DMA((19,)),
            ]
        else:
            body_of = functools.partial(kernel, nx, nz, nl, nxl)
            scratch = block + [
                pltpu.VMEM((2, rows, ny), f32),
                pltpu.VMEM((rows, ny), jnp.int32),
                pltpu.VMEM((nxl, ny), f32),
                pltpu.VMEM((nl, nxl, ny), f32),
                pltpu.VMEM((4, rows, ny), f32),
                pltpu.VMEM((rows, ny), f32),
                pltpu.VMEM((3, rows, ny), f32),
                pltpu.VMEM((nz - 1, 3, rows, ny), f32),
                pltpu.SemaphoreType.DMA((7,)),
                pltpu.SemaphoreType.DMA((12,)),
                pltpu.SemaphoreType.DMA((12,)),
                pltpu.SemaphoreType.DMA((nz - 1,)),
                pltpu.SemaphoreType.DMA((nz - 1,)),
            ]
        held, fresh, weight = pl.pallas_call(
            body_of,
            out_shape=(
                pltpu.VMEM((4, nl, rows, ny), f32),
                pltpu.VMEM(thickness.shape, f32),
                pltpu.VMEM(density.shape, f32),
            ),
            in_specs=[pl.BlockSpec(memory_space=pl.ANY)] * 7,
            out_specs=(vmem, vmem, vmem),
            scratch_shapes=scratch,
            compiler_params=pltpu.CompilerParams(collective_id=0, has_side_effects=True),
        )(flow, fluid, density, thickness, bed, smb, mask)
        anywhere = pl.BlockSpec(memory_space=pl.ANY)
        return pl.pallas_call(
            functools.partial(write, nxl),
            out_shape=(
                jax.ShapeDtypeStruct(flow.shape, f32),
                jax.ShapeDtypeStruct(thickness.shape, f32),
                jax.ShapeDtypeStruct(density.shape, f32),
            ),
            in_specs=[vmem] * 3,
            out_specs=(anywhere,) * 3,
            scratch_shapes=[pltpu.SemaphoreType.DMA((3,))],
        )(*(pltpu.with_memory_space_constraint(x, pltpu.VMEM) for x in (held, fresh, weight)))

    placed = (
        P(None, "gz", "gx", None), P("gz", "gx", None), P("gz", "gx", None),
        P("gx", None), P("gx", None), P("gx", None), P("gx", None),
    )
    return jax.shard_map(
        body, mesh=mesh, in_specs=placed,
        out_specs=(P(None, "gz", "gx", None), P("gx", None), P("gz", "gx", None)),
        check_vma=False,
    )
```

```python
import functools

import jax
import jax.numpy as jnp
from jax import lax
from jax.experimental import pallas as pl
from jax.experimental.pallas import tpu as pltpu
from jax.sharding import PartitionSpec as P

REGULAR = 0.01
FRICTION = 2.0
STEP = 0.2
TIME_STEP = 0.5

XH = 5
ZH = 4
PAD = 16
MESH = pl.DeviceIdType.MESH


def kernel(nx, nz, nl, nxl, flow, fluid, density, thickness, bed, smb, mask,
           flow_out, new_thickness, overburden,
           S0, S1, T, V, G, M, SM, DN, A, FX, FS, FR,
           loc, send, recv, fsend, frecv):
    gx, gz = lax.axis_index("gx"), lax.axis_index("gz")
    left, right = lax.rem(gx + nx - 1, nx), lax.rem(gx + 1, nx)
    down, up = lax.rem(gz + nz - 1, nz), lax.rem(gz + 1, nz)
    has_left, has_right = gx > 0, gx < nx - 1
    has_down, has_up = gz > 0, gz < nz - 1
    ny = flow.shape[-1]
    levels_total = nl * nz
    depth, rows = S0.shape[1], S0.shape[2]
    if nz == 2:
        base = 1 + ZH * gz
        base_up, base_down = 1 + ZH, 1

        def span(h):
            return base - h * gz, nl + h
    else:
        base = base_up = base_down = 1 + ZH

        def span(h):
            return base - h, nl + 2 * h

    own = pl.ds(base, nl)
    mine = slice(PAD, PAD + nxl)
    lo, hi = PAD - 8, PAD + nxl + 8
    c, m, p = slice(lo, hi), slice(lo - 1, hi - 1), slice(lo + 1, hi + 1)
    width = hi - lo

    copies = [
        pltpu.make_async_copy(flow, S0.at[pl.ds(0, 4), own, mine], loc.at[0]),
        pltpu.make_async_copy(fluid, S0.at[4, own, mine], loc.at[1]),
        pltpu.make_async_copy(thickness, G.at[0, mine], loc.at[2]),
        pltpu.make_async_copy(bed, G.at[1, mine], loc.at[3]),
        pltpu.make_async_copy(mask, M.at[mine], loc.at[4]),
        pltpu.make_async_copy(density, DN, loc.at[5]),
        pltpu.make_async_copy(smb, SM, loc.at[6]),
    ]
    for copy in copies:
        copy.start()

    barrier = pltpu.get_barrier_semaphore()

    @pl.when(has_left)
    def _():
        pl.semaphore_signal(barrier, inc=1, device_id={"gx": left}, device_id_type=MESH)

    @pl.when(has_right)
    def _():
        pl.semaphore_signal(barrier, inc=1, device_id={"gx": right}, device_id_type=MESH)

    for off in range(1, nz):
        pl.semaphore_signal(barrier, inc=1, device_id={"gz": lax.rem(gz + off, nz)}, device_id_type=MESH)

    zrow = jnp.zeros((rows, ny), jnp.float32)
    for k in (0, depth - 1):
        for f in range(4):
            S0[f, k] = zrow
            S1[f, k] = zrow
        for f in range(3):
            T[f, k] = zrow

    def outside_x(where):
        strip = slice(PAD - 8, PAD) if where == 0 else slice(PAD + nxl, PAD + nxl + 8)
        zero = jnp.zeros((8, ny), jnp.float32)

        def one(k, _):
            for f in range(4):
                S0[f, k, strip] = zero
            S0[4, k, strip] = zero + 1.0
            return 0

        lax.fori_loop(1, depth - 1, one, 0)
        G[0, strip] = zero
        G[1, strip] = zero
        M[strip] = jnp.zeros((8, ny), jnp.int32)

    @pl.when(jnp.logical_not(has_left))
    def _():
        outside_x(0)

    @pl.when(jnp.logical_not(has_right))
    def _():
        outside_x(1)

    if nz > 2:
        def outside_z(start):
            for k in range(start, start + ZH):
                for f in range(4):
                    S0[f, k, c] = jnp.zeros((width, ny), jnp.float32)
                S0[4, k, c] = jnp.ones((width, ny), jnp.float32)

        @pl.when(jnp.logical_not(has_down))
        def _():
            outside_z(1)

        @pl.when(jnp.logical_not(has_up))
        def _():
            outside_z(1 + ZH + nl)

    def remote(src, dst, number, device):
        return pltpu.make_async_remote_copy(src_ref=src, dst_ref=dst, send_sem=send.at[number],
                                            recv_sem=recv.at[number], device_id=device, device_id_type=MESH)

    first, last = pl.ds(PAD, XH), pl.ds(PAD + nxl - XH, XH)
    from_left, from_right = pl.ds(PAD - XH, XH), pl.ds(PAD + nxl, XH)
    every = pl.ds(0, 5)
    leftward = [
        remote(S0.at[every, own, first], S0.at[every, own, from_right], 0, {"gx": left}),
        remote(G.at[:, first], G.at[:, from_right], 1, {"gx": left}),
        remote(M.at[first], M.at[from_right], 2, {"gx": left}),
    ]
    rightward = [
        remote(S0.at[every, own, last], S0.at[every, own, from_left], 3, {"gx": right}),
        remote(G.at[:, last], G.at[:, from_left], 4, {"gx": right}),
        remote(M.at[last], M.at[from_left], 5, {"gx": right}),
    ]
    top, bottom = pl.ds(base + nl - ZH, ZH), pl.ds(base, ZH)
    from_down, from_up = pl.ds(base_up - ZH, ZH), pl.ds(base_down + nl, ZH)
    pieces = (pl.ds(PAD, nxl), from_left, from_right)
    upward = [remote(S0.at[every, top, piece], S0.at[every, from_down, piece], 6 + n, {"gz": up})
              for n, piece in enumerate(pieces)]
    downward = [remote(S0.at[every, bottom, piece], S0.at[every, from_up, piece], 9 + n, {"gz": down})
                for n, piece in enumerate(pieces)]

    for n in range(5):
        copies[n].wait()
    pl.semaphore_wait(barrier, nz - 1 + jnp.where(has_left, 1, 0) + jnp.where(has_right, 1, 0))

    @pl.when(has_left)
    def _():
        for copy in leftward:
            copy.start()

    @pl.when(has_right)
    def _():
        for copy in rightward:
            copy.start()

    @pl.when(has_up)
    def _():
        upward[0].start()

    @pl.when(has_down)
    def _():
        downward[0].start()

    copies[5].wait()
    copies[6].wait()
    total = jnp.zeros((nxl, ny), jnp.float32)
    for k in reversed(range(nl)):
        cell = DN[k]
        DN[k] = total + 0.5 * cell
        total = total + cell
    FS[2, mine] = total

    def dy(f):
        axis = f.ndim - 1
        lane = lax.broadcasted_iota(jnp.int32, f.shape, axis)
        return (jnp.where(lane < ny - 1, pltpu.roll(f, ny - 1, axis), 0.0)
                - jnp.where(lane > 0, pltpu.roll(f, 1, axis), 0.0))

    def inside(start, height):
        column = gx * nxl + lax.broadcasted_iota(jnp.int32, (height, ny), 0) + (start - PAD)
        return (column >= 0) & (column < nx * nxl)

    def plan(start, height):
        c = slice(start, start + height)
        A[0, c] = 0.5 * (FX[start + 1:start + height + 1] - FX[start - 1:start + height - 1])
        A[1, c] = 0.5 * dy(FX[c])
        A[2, c] = jnp.where(inside(start, height) & (M[c] > 0), 1.0, 0.0)
        A[3, c] = jnp.where(M[c] == 1, FRICTION, 0.0)

    def level_at(k, count):
        return gz * nl + k - base + lax.broadcasted_iota(jnp.int32, (count, 1, ny), 0)

    def stress(B, k, count, start, height):
        at = pl.ds(k, count)
        c = slice(start, start + height)
        m, p = slice(start - 1, start + height - 1), slice(start + 1, start + height + 1)
        above, below = pl.ds(k + 1, count), pl.ds(k - 1, count)
        xx, vx, wx = (B[f, at, p] - B[f, at, m] for f in range(3))
        uz, vz, zz = (B[f, above, c] - B[f, below, c] for f in range(3))
        uy, yy, wy = (dy(B[f, at, c]) for f in range(3))
        xy, xz, yz = uy + vx, uz + wx, vz + wy
        twice = xx * xx + yy * yy + zz * zz
        second = 0.0625 * (twice + twice + (xy * xy + xz * xz + yz * yz))
        third = jnp.log2(S0[4, at, c] * (second + REGULAR)) * (1.0 / 3.0)
        a = jnp.exp2(-third)
        V[0, at, c] = (2.0 * STEP) * jnp.exp2(third)
        V[1, at, c] = (0.25 * STEP) * a * (xx + yy + zz)
        h = 0.25 * a
        if height == 8:
            h = jnp.where(jnp.broadcast_to(inside(start, height)[None], h.shape), h, 0.0)
        if nz > 2:
            level = level_at(k, count)
            ok = jnp.where((level >= 0) & (level < levels_total), 1.0, 0.0)
            h = jnp.where(jnp.broadcast_to(ok, h.shape) > 0.0, h, 0.0)
        g = 0.5 * h
        T[0, at, c] = g * xz
        T[1, at, c] = g * yz
        T[2, at, c] = h * zz
        T[3, at, c] = h * xx
        T[4, at, c] = g * xy
        T[5, at, c] = h * yy

    def move(B, k, count, start, height):
        at = pl.ds(k, count)
        c = slice(start, start + height)
        m, p = slice(start - 1, start + height - 1), slice(start + 1, start + height + 1)
        above, below = pl.ds(k + 1, count), pl.ds(k - 1, count)
        level = level_at(k, count)
        drag = jnp.where(level == 0, 1.0, 0.0) * A[3, c][None]
        u, v, press = B[0, at, c], B[1, at, c], B[3, at, c]
        fx = ((T[3, at, p] - T[3, at, m]) + dy(T[4, at, c]) + (T[0, above, c] - T[0, below, c])
              - 0.5 * (B[3, at, p] - B[3, at, m]) - A[0, c][None] - drag * u)
        fy = ((T[4, at, p] - T[4, at, m]) + dy(T[5, at, c]) + (T[1, above, c] - T[1, below, c])
              - 0.5 * dy(press) - A[1, c][None] - drag * v)
        fz = ((T[0, at, p] - T[0, at, m]) + dy(T[1, at, c]) + (T[2, above, c] - T[2, below, c])
              - 0.5 * (B[3, above, c] - B[3, below, c]))
        step = V[0, at, c]
        ice = jnp.broadcast_to(A[2, c][None], u.shape)
        if nz > 2:
            ice = ice * jnp.where((level >= 0) & (level < levels_total), 1.0, 0.0)
        return [jnp.where(ice > 0.0, value, 0.0) for value in (
            u + step * fx, v + step * fy, B[2, at, c] + step * fz, press - V[1, at, c])]

    def blocks(reach, most, step, areas):
        start, count = span(reach)
        pieces = -(-count // most)
        for n in range(pieces):
            one, two = count * n // pieces, count * (n + 1) // pieces
            for area in areas:
                step(start + one, two - one, *area)

    def stress_first(*at):
        stress(S0, *at)

    def stress_last(*at):
        stress(S1, *at)

    def move_first(k, count, start, height):
        for f, value in enumerate(move(S0, k, count, start, height)):
            S1[f, pl.ds(k, count), start:start + height] = value

    def move_last(k, count, start, height):
        for f, value in enumerate(move(S1, k, count, start, height)):
            flow_out[f, pl.ds(k - base, count), start:start + height] = value

    middle = [(PAD + 1, nxl - 2)]
    FX[mine] = G[1, mine] + G[0, mine]
    plan(*middle[0])
    for flag, group in ((has_down, upward), (has_up, downward)):
        @pl.when(flag)
        def _():
            group[0].wait_recv()

    blocks(3, 2, stress_first, middle)
    blocks(2, 2, move_first, middle)
    blocks(1, 2, stress_last, middle)

    @pl.when(has_left)
    def _():
        for copy in rightward:
            copy.wait_recv()

    @pl.when(has_left & has_up)
    def _():
        upward[1].start()

    @pl.when(has_left & has_down)
    def _():
        downward[1].start()

    @pl.when(has_right)
    def _():
        for copy in leftward:
            copy.wait_recv()

    @pl.when(has_right & has_up)
    def _():
        upward[2].start()

    @pl.when(has_right & has_down)
    def _():
        downward[2].start()

    blocks(0, 2, move_last, middle)

    ends = [(PAD - 4, 8), (PAD + nxl - 4, 8)]
    for start in (PAD - 8, PAD + nxl):
        strip = slice(start, start + 8)
        FX[strip] = G[1, strip] + G[0, strip]
    for area in ends:
        plan(*area)
    for flag, group in ((has_down, upward), (has_up, downward)):
        @pl.when(flag & has_left)
        def _():
            group[1].wait_recv()

        @pl.when(flag & has_right)
        def _():
            group[2].wait_recv()

    blocks(3, 6, stress_first, ends)
    blocks(2, 6, move_first, [(PAD - 5, 8), (PAD + nxl - 3, 8)])
    blocks(1, 6, stress_last, ends)
    blocks(0, 4, move_last, ends)
    sum_u, sum_v = flow_out[0, 0, c], flow_out[1, 0, c]
    for k in range(1, nl):
        sum_u = sum_u + flow_out[0, k, c]
        sum_v = sum_v + flow_out[1, k, c]
    FS[0, c] = sum_u
    FS[1, c] = sum_v

    sums = [pltpu.make_async_remote_copy(
        src_ref=FS.at[:, pl.ds(lo, width)], dst_ref=FR.at[off - 1, :, pl.ds(lo, width)],
        send_sem=fsend.at[off - 1], recv_sem=frecv.at[off - 1],
        device_id={"gz": lax.rem(gz + off, nz)}, device_id_type=MESH) for off in range(1, nz)]
    for copy in sums:
        copy.start()
    above = jnp.zeros((nxl, ny), jnp.float32)
    for off in range(1, nz):
        sums[off - 1].wait_recv()
        sum_u = sum_u + FR[off - 1, 0, c]
        sum_v = sum_v + FR[off - 1, 1, c]
        above = above + jnp.where(gz < off, 1.0, 0.0) * FR[off - 1, 2, mine]
    part = G[0, c] * (1.0 / levels_total)
    FX[c] = part * sum_u
    flux_y = dy(part * sum_v)[8:8 + nxl]
    spread = FX[PAD + 1:PAD + nxl + 1] - FX[PAD - 1:PAD + nxl - 1] + flux_y
    fresh = G[0, mine] + TIME_STEP * (SM[...] - 0.5 * spread)
    new_thickness[...] = fresh
    weight = fresh * (1.0 / levels_total)
    for k in range(nl):
        overburden[k] = weight * (above + DN[k])

    @pl.when(has_left)
    def _():
        for copy in leftward:
            copy.wait_send()

    @pl.when(has_right)
    def _():
        for copy in rightward:
            copy.wait_send()

    for flag, group in ((has_up, upward), (has_down, downward)):
        @pl.when(flag)
        def _():
            group[0].wait_send()

        @pl.when(flag & has_left)
        def _():
            group[1].wait_send()

        @pl.when(flag & has_right)
        def _():
            group[2].wait_send()

    for copy in sums:
        copy.wait_send()


def paired(nx, nl, nxl, flow, fluid, density, thickness, bed, smb, mask,
           flow_out, new_thickness, overburden,
           S0, S1, T, V, G, M, PK, RK, SM, DN, A, FX, FM, RM, FE, RE, FD, RD,
           loc, send, recv):
    gx, gz = lax.axis_index("gx"), lax.axis_index("gz")
    left, right = lax.rem(gx + nx - 1, nx), lax.rem(gx + 1, nx)
    has_left, has_right = gx > 0, gx < nx - 1
    odd = lax.rem(gx, 2)
    near = gx + 1 - 2 * odd
    far = lax.rem(gx + nx - 1 + 2 * odd, nx)
    has_far = jnp.where(odd == 1, gx, nx - 1 - gx) < nx - 1
    ny = flow.shape[-1]
    levels_total = 2 * nl
    depth, rows = S0.shape[1], S0.shape[2]
    base = 1 + ZH * gz
    own = pl.ds(base, nl)
    facing = pl.ds(1 + nl - ZH + gz * (2 * ZH - nl), ZH)
    others = pl.ds(1 + gz * 2 * ZH, nl - ZH)
    across = pl.ds(1 + gz * nl, ZH)
    mine = slice(PAD, PAD + nxl)

    barrier = pltpu.get_barrier_semaphore()
    pl.semaphore_signal(barrier, inc=1, device_id={"gx": near}, device_id_type=MESH)
    pl.semaphore_signal(barrier, inc=1, device_id={"gz": 1 - gz}, device_id_type=MESH)

    @pl.when(has_far)
    def _():
        pl.semaphore_signal(barrier, inc=1, device_id={"gx": far}, device_id_type=MESH)

    copies = [
        pltpu.make_async_copy(flow, S0.at[pl.ds(0, 4), own, mine], loc.at[0]),
        pltpu.make_async_copy(fluid, S0.at[4, own, mine], loc.at[1]),
        pltpu.make_async_copy(thickness, G.at[0, mine], loc.at[2]),
        pltpu.make_async_copy(bed, G.at[1, mine], loc.at[3]),
        pltpu.make_async_copy(mask, M, loc.at[4]),
        pltpu.make_async_copy(density, DN, loc.at[5]),
        pltpu.make_async_copy(smb, SM, loc.at[6]),
    ]
    for copy in copies:
        copy.start()

    zrow = jnp.zeros((rows, ny), jnp.float32)
    for k in (0, depth - 1):
        for f in range(4):
            S0[f, k] = zrow
            S1[f, k] = zrow
        for f in range(3):
            T[f, k] = zrow

    def outside_x(where):
        strip = slice(PAD - 8, PAD) if where == 0 else slice(PAD + nxl, PAD + nxl + 8)
        zero = jnp.zeros((8, ny), jnp.float32)

        def one(k, _):
            for f in range(4):
                S0[f, k, strip] = zero
            S0[4, k, strip] = zero + 1.0
            return 0

        lax.fori_loop(1, depth - 1, one, 0)
        G[0, strip] = zero
        G[2, strip] = zero
        FX[strip] = zero

    @pl.when(jnp.logical_not(has_left))
    def _():
        outside_x(0)

    @pl.when(jnp.logical_not(has_right))
    def _():
        outside_x(1)

    def remote(src, dst, number, device):
        return pltpu.make_async_remote_copy(src_ref=src, dst_ref=dst, send_sem=send.at[number],
                                            recv_sem=recv.at[number], device_id=device, device_id_type=MESH)

    motion, state = pl.ds(0, 3), pl.ds(3, 2)

    def halo(levels, src, dst, number, device):
        (src_uvw, src_pf), (dst_uvw, dst_pf) = src, dst
        return [remote(S0.at[motion, levels, src_uvw], S0.at[motion, levels, dst_uvw], number, device),
                remote(S0.at[state, levels, src_pf], S0.at[state, levels, dst_pf], number + 1, device)]

    first = pl.ds(PAD, XH), pl.ds(PAD, XH - 1)
    last = pl.ds(PAD + nxl - XH, XH), pl.ds(PAD + nxl - XH + 1, XH - 1)
    from_left = pl.ds(PAD - XH, XH), pl.ds(PAD - XH + 1, XH - 1)
    from_right = pl.ds(PAD + nxl, XH), pl.ds(PAD + nxl, XH - 1)

    def sideways(src, dst, side, number, device):
        early = halo(facing, src, dst, number, device)
        early.append(remote(PK.at[side], RK.at[1 - side], number + 2, device))
        return early, halo(others, src, dst, number + 3, device)

    leftward = sideways(first, from_right, 0, 0, {"gx": left})
    rightward = sideways(last, from_left, 1, 5, {"gx": right})
    partner = {"gz": 1 - gz}
    planes = remote(S0.at[pl.ds(0, 5), facing, pl.ds(PAD, nxl)], S0.at[pl.ds(0, 5), across, pl.ds(PAD, nxl)], 10, partner)

    def corner(at, number):
        (uvw, pf) = at
        return [remote(S0.at[motion, facing, uvw], S0.at[motion, across, uvw], number, partner),
                remote(S0.at[state, facing, pf], S0.at[state, across, pf], number + 1, partner)]

    corners = corner(from_left, 11), corner(from_right, 13)
    weights = remote(FD, RD, 15, partner)
    inner = remote(FM, RM, 16, partner)
    strips = [remote(FE.at[side], RE.at[side], 17 + side, partner) for side in range(2)]
    incoming = rightward, leftward
    have = (has_left, has_right)

    for n in range(5):
        copies[n].wait()
    G[2, mine] = M[...].astype(jnp.float32)
    FX[mine] = G[1, mine] + G[0, mine]
    end = PAD + nxl
    PK[0, 0:4] = FX[PAD:PAD + 4]
    PK[0, 4:7] = G[2, PAD:PAD + 3]
    PK[0, 7:8] = G[0, PAD:PAD + 1]
    PK[1, 0:4] = FX[end - 4:end]
    PK[1, 4:7] = G[2, end - 3:end]
    PK[1, 7:8] = G[0, end - 1:end]

    pl.semaphore_wait(barrier, 2 + jnp.where(has_far, 1, 0))

    def launch(group, flag):
        @pl.when(flag)
        def _():
            for copy in group:
                copy.start()

    launch(leftward[0], odd == 1)
    launch(rightward[0], odd == 0)
    eager = lax.rem(gx + 1, 4) < 2
    launch(leftward[1], (odd == 1) & eager)
    launch(rightward[1], (odd == 0) & eager)
    planes.start()

    launch(rightward[0], (odd == 1) & has_right)
    launch(leftward[0], (odd == 0) & has_left)
    launch(leftward[1], (odd == 1) & jnp.logical_not(eager))
    launch(rightward[1], (odd == 0) & jnp.logical_not(eager))
    launch(rightward[1], (odd == 1) & has_right)
    launch(leftward[1], (odd == 0) & has_left)


    def dy(f):
        axis = f.ndim - 1
        lane = lax.broadcasted_iota(jnp.int32, f.shape, axis)
        return (jnp.where(lane < ny - 1, pltpu.roll(f, ny - 1, axis), 0.0)
                - jnp.where(lane > 0, pltpu.roll(f, 1, axis), 0.0))

    def inside(start, height):
        column = gx * nxl + lax.broadcasted_iota(jnp.int32, (height, ny), 0) + (start - PAD)
        return (column >= 0) & (column < nx * nxl)

    def plan(start, height):
        c = slice(start, start + height)
        A[0, c] = 0.5 * (FX[start + 1:start + height + 1] - FX[start - 1:start + height - 1])
        A[1, c] = 0.5 * dy(FX[c])
        A[2, c] = jnp.where(inside(start, height) & (G[2, c] > 0.0), 1.0, 0.0)
        A[3, c] = jnp.where(G[2, c] == 1.0, FRICTION, 0.0)

    def level_at(k, count):
        return gz * nl + k - base + lax.broadcasted_iota(jnp.int32, (count, 1, ny), 0)

    def stress(B, k, count, start, height):
        at = pl.ds(k, count)
        c = slice(start, start + height)
        m, p = slice(start - 1, start + height - 1), slice(start + 1, start + height + 1)
        above, below = pl.ds(k + 1, count), pl.ds(k - 1, count)
        xx, vx, wx = (B[f, at, p] - B[f, at, m] for f in range(3))
        uz, vz, zz = (B[f, above, c] - B[f, below, c] for f in range(3))
        uy, yy, wy = (dy(B[f, at, c]) for f in range(3))
        xy, xz, yz = uy + vx, uz + wx, vz + wy
        twice = xx * xx + yy * yy + zz * zz
        second = 0.0625 * (twice + twice + (xy * xy + xz * xz + yz * yz))
        third = jnp.log2(S0[4, at, c] * (second + REGULAR)) * (1.0 / 3.0)
        a = jnp.exp2(-third)
        V[0, at, c] = (2.0 * STEP) * jnp.exp2(third)
        V[1, at, c] = (0.25 * STEP) * a * (xx + yy + zz)
        h = 0.25 * a
        if height == 8:
            h = jnp.where(jnp.broadcast_to(inside(start, height)[None], h.shape), h, 0.0)
        g = 0.5 * h
        q = 0.5 * B[3, at, c]
        T[0, at, c] = g * xz
        T[1, at, c] = g * yz
        T[2, at, c] = h * zz - q
        T[3, at, c] = h * xx - q
        T[4, at, c] = g * xy
        T[5, at, c] = h * yy - q

    def move(B, k, count, start, height):
        at = pl.ds(k, count)
        c = slice(start, start + height)
        m, p = slice(start - 1, start + height - 1), slice(start + 1, start + height + 1)
        above, below = pl.ds(k + 1, count), pl.ds(k - 1, count)
        drag = jnp.where(level_at(k, count) == 0, 1.0, 0.0) * A[3, c][None]
        u, v, press = B[0, at, c], B[1, at, c], B[3, at, c]
        fx = ((T[3, at, p] - T[3, at, m]) + dy(T[4, at, c]) + (T[0, above, c] - T[0, below, c])
              - A[0, c][None] - drag * u)
        fy = ((T[4, at, p] - T[4, at, m]) + dy(T[5, at, c]) + (T[1, above, c] - T[1, below, c])
              - A[1, c][None] - drag * v)
        fz = ((T[0, at, p] - T[0, at, m]) + dy(T[1, at, c]) + (T[2, above, c] - T[2, below, c]))
        step = V[0, at, c]
        ice = jnp.broadcast_to(A[2, c][None], u.shape)
        return [jnp.where(ice > 0.0, value, 0.0) for value in (
            u + step * fx, v + step * fy, B[2, at, c] + step * fz, press - V[1, at, c])]

    def blocks(start, count, most, step, area):
        pieces = -(-count // most)
        for n in range(pieces):
            one, two = count * n // pieces, count * (n + 1) // pieces
            step(start + one, two - one, *area)

    def apart(reach, most, step, area):
        blocks(1 + gz * (2 * ZH - reach), nl - ZH + reach, most, step, area)

    def facing_part(reach, most, step, area):
        low, high = 1 + nl - ZH + reach, 1 + ZH - reach
        blocks(low + gz * (high - low), ZH, most, step, area)

    def reached(reach, most, step, area):
        low = 1 + nl - reach
        blocks(low + gz * (1 + ZH - reach - low), 2 * (ZH - 4 + reach), most, step, area)

    def rest(reach, most, step, area):
        count = nl - reach
        blocks(1 + gz * (ZH + nl - count), count, most, step, area)

    def stress_first(*at):
        stress(S0, *at)

    def stress_last(*at):
        stress(S1, *at)

    def move_first(k, count, start, height):
        for f, value in enumerate(move(S0, k, count, start, height)):
            S1[f, pl.ds(k, count), start:start + height] = value

    def move_last(k, count, start, height):
        for f, value in enumerate(move(S1, k, count, start, height)):
            flow_out[f, pl.ds(k - base, count), start:start + height] = value

    middle = (PAD + 1, nxl - 2)
    plan(*middle)
    apart(3, 2, stress_first, middle)

    copies[5].wait()
    copies[6].wait()
    total = jnp.zeros((nxl, ny), jnp.float32)
    for k in reversed(range(nl)):
        cell = DN[k]
        DN[k] = total + 0.5 * cell
        total = total + cell
    FD[...] = total
    weights.start()

    apart(2, 2, move_first, middle)
    apart(1, 2, stress_last, middle)
    apart(0, 2, move_last, middle)
    planes.wait_recv()
    facing_part(3, 2, stress_first, middle)

    def forward(side):
        @pl.when(have[side])
        def _():
            for copy in incoming[side][0][:2]:
                copy.wait_recv()
            for copy in corners[side]:
                copy.start()

    place = lax.rem(gx, 4)
    crossed = ((place == 2) & (gx > 2)) | ((place == 1) & (gx > 1) & (gx < nx - 3))
    left_leads = (gx == 0) | (((odd == 1) != crossed) & has_right)

    def by_arrival(step):
        @pl.when(left_leads)
        def _():
            step(0, 1)

        @pl.when(jnp.logical_not(left_leads))
        def _():
            step(1, 0)

    facing_part(2, 2, move_first, middle)
    facing_part(1, 2, stress_last, middle)
    facing_part(0, 2, move_last, middle)

    by_arrival(lambda lead, other: forward(lead))

    def depth_sum(f, c):
        value = flow_out[f, 0, c]
        for k in range(1, nl):
            value = value + flow_out[f, k, c]
        return value

    for f in range(2):
        FM[f] = depth_sum(f, mine)
    inner.start()

    edges = [((PAD - 4, 8), (PAD - 5, 8)), ((PAD + nxl - 4, 8), (PAD + nxl - 3, 8))]

    def approach(side):
        area, shifted = edges[side]

        @pl.when(have[side])
        def _():
            incoming[side][0][2].wait_recv()
            at = PAD if side == 0 else end
            for row in range(4):
                to = at - 4 + row if side == 0 else at + row
                FX[to:to + 1] = RK[side, row:row + 1]
            for row in range(3):
                to = at - 3 + row if side == 0 else at + row
                G[2, to:to + 1] = RK[side, 4 + row:5 + row]
            to = at - 1 if side == 0 else at
            G[0, to:to + 1] = RK[side, 7:8]
            for copy in corners[side]:
                copy.wait_recv()

        plan(*area)
        reached(3, 3, stress_first, area)
        reached(2, 4, move_first, shifted)
        reached(1, 4, stress_last, area)

    def finish(side):
        area, shifted = edges[side]

        @pl.when(have[side])
        def _():
            for copy in incoming[side][1]:
                copy.wait_recv()

        rest(3, 5, stress_first, area)
        rest(2, 6, move_first, shifted)
        rest(1, 4, stress_last, area)
        rest(0, 4, move_last, area)
        wide = slice(PAD - 8, PAD + 8) if side == 0 else slice(PAD + nxl - 8, PAD + nxl + 8)
        for f in range(2):
            FE[side, f] = depth_sum(f, wide)
        strips[side].start()

    def both(lead, other):
        forward(other)
        approach(lead)
        finish(lead)
        approach(other)
        finish(other)

    by_arrival(both)

    def settle(start, height, sum_v):
        c = slice(start, start + height)
        o = slice(start - PAD, start - PAD + height)
        flux_y = dy(G[0, c] * (1.0 / levels_total) * sum_v)
        spread = FX[start + 1:start + height + 1] - FX[start - 1:start + height - 1] + flux_y
        fresh = G[0, c] + TIME_STEP * (SM[o] - 0.5 * spread)
        new_thickness[o] = fresh
        weight = fresh * (1.0 / levels_total)
        above = jnp.where(gz == 0, 1.0, 0.0) * RD[o]
        for k in range(nl):
            overburden[k, o] = weight * (above + DN[k, o])

    weights.wait_recv()
    inner.wait_recv()
    FX[mine] = G[0, mine] * (1.0 / levels_total) * (FM[0] + RM[0])
    settle(PAD + 8, nxl - 16, FM[1, 8:nxl - 8] + RM[1, 8:nxl - 8])
    for side in range(2):
        strips[side].wait_recv()
        begin = PAD - 8 if side == 0 else PAD + nxl - 8
        wide = slice(begin, begin + 16)
        FX[wide] = G[0, wide] * (1.0 / levels_total) * (FE[side, 0] + RE[side, 0])
        inward = slice(8, 16) if side == 0 else slice(0, 8)
        settle(PAD if side == 0 else PAD + nxl - 8, 8, FE[side, 1, inward] + RE[side, 1, inward])

    for side, group in ((0, leftward), (1, rightward)):
        @pl.when(have[side])
        def _():
            for copy in (*group[0], *group[1], *corners[side]):
                copy.wait_send()

    for copy in (planes, weights, inner, *strips):
        copy.wait_send()


def write(nxl, held, fresh, weight, flow_out, new_thickness, overburden, done):
    copies = [
        pltpu.make_async_copy(held.at[:, :, pl.ds(PAD, nxl)], flow_out, done.at[0]),
        pltpu.make_async_copy(fresh, new_thickness, done.at[1]),
        pltpu.make_async_copy(weight, overburden, done.at[2]),
    ]
    for copy in copies:
        copy.start()
    for copy in copies:
        copy.wait()


def solution(mesh):
    nx, nz = mesh.shape["gx"], mesh.shape["gz"]

    def body(flow, fluid, density, thickness, bed, smb, mask):
        nl, nxl, ny = fluid.shape
        depth = nl + 2 + (ZH if nz == 2 else 2 * ZH)
        rows = nxl + 2 * PAD
        f32 = jnp.float32
        vmem = pl.BlockSpec(memory_space=pltpu.VMEM)
        block = [pltpu.VMEM((n, depth, rows, ny), f32) for n in (5, 4, 6, 2)]
        if nz == 2 and nx % 2 == 0 and nl > ZH and nxl >= 24:
            body_of = functools.partial(paired, nx, nl, nxl)
            scratch = block + [
                pltpu.VMEM((3, rows, ny), f32),
                pltpu.VMEM((nxl, ny), jnp.int32),
                pltpu.VMEM((2, 8, ny), f32),
                pltpu.VMEM((2, 8, ny), f32),
                pltpu.VMEM((nxl, ny), f32),
                pltpu.VMEM((nl, nxl, ny), f32),
                pltpu.VMEM((4, rows, ny), f32),
                pltpu.VMEM((rows, ny), f32),
                pltpu.VMEM((2, nxl, ny), f32),
                pltpu.VMEM((2, nxl, ny), f32),
                pltpu.VMEM((2, 2, 16, ny), f32),
                pltpu.VMEM((2, 2, 16, ny), f32),
                pltpu.VMEM((nxl, ny), f32),
                pltpu.VMEM((nxl, ny), f32),
                pltpu.SemaphoreType.DMA((7,)),
                pltpu.SemaphoreType.DMA((19,)),
                pltpu.SemaphoreType.DMA((19,)),
            ]
        else:
            body_of = functools.partial(kernel, nx, nz, nl, nxl)
            scratch = block + [
                pltpu.VMEM((2, rows, ny), f32),
                pltpu.VMEM((rows, ny), jnp.int32),
                pltpu.VMEM((nxl, ny), f32),
                pltpu.VMEM((nl, nxl, ny), f32),
                pltpu.VMEM((4, rows, ny), f32),
                pltpu.VMEM((rows, ny), f32),
                pltpu.VMEM((3, rows, ny), f32),
                pltpu.VMEM((nz - 1, 3, rows, ny), f32),
                pltpu.SemaphoreType.DMA((7,)),
                pltpu.SemaphoreType.DMA((12,)),
                pltpu.SemaphoreType.DMA((12,)),
                pltpu.SemaphoreType.DMA((nz - 1,)),
                pltpu.SemaphoreType.DMA((nz - 1,)),
            ]
        held, fresh, weight = pl.pallas_call(
            body_of,
            out_shape=(
                pltpu.VMEM((4, nl, rows, ny), f32),
                pltpu.VMEM(thickness.shape, f32),
                pltpu.VMEM(density.shape, f32),
            ),
            in_specs=[pl.BlockSpec(memory_space=pl.ANY)] * 7,
            out_specs=(vmem, vmem, vmem),
            scratch_shapes=scratch,
            compiler_params=pltpu.CompilerParams(collective_id=0, has_side_effects=True),
        )(flow, fluid, density, thickness, bed, smb, mask)
        anywhere = pl.BlockSpec(memory_space=pl.ANY)
        return pl.pallas_call(
            functools.partial(write, nxl),
            out_shape=(
                jax.ShapeDtypeStruct(flow.shape, f32),
                jax.ShapeDtypeStruct(thickness.shape, f32),
                jax.ShapeDtypeStruct(density.shape, f32),
            ),
            in_specs=[vmem] * 3,
            out_specs=(anywhere,) * 3,
            scratch_shapes=[pltpu.SemaphoreType.DMA((3,))],
        )(*(pltpu.with_memory_space_constraint(x, pltpu.VMEM) for x in (held, fresh, weight)))

    placed = (
        P(None, "gz", "gx", None), P("gz", "gx", None), P("gz", "gx", None),
        P("gx", None), P("gx", None), P("gx", None), P("gx", None),
    )
    return jax.shard_map(
        body, mesh=mesh, in_specs=placed,
        out_specs=(P(None, "gz", "gx", None), P("gx", None), P("gz", "gx", None)),
        check_vma=False,
    )
```

```python
import functools

import jax
import jax.numpy as jnp
from jax import lax
from jax.experimental import pallas as pl
from jax.experimental.pallas import tpu as pltpu
from jax.sharding import PartitionSpec as P

REGULAR = 0.01
FRICTION = 2.0
STEP = 0.2
TIME_STEP = 0.5

XH = 5
ZH = 4
PAD = 16
MESH = pl.DeviceIdType.MESH


def kernel(nx, nz, nl, nxl, flow, fluid, density, thickness, bed, smb, mask,
           flow_out, new_thickness, overburden,
           S0, S1, T, V, G, M, SM, DN, A, FX, FS, FR,
           loc, send, recv, fsend, frecv):
    gx, gz = lax.axis_index("gx"), lax.axis_index("gz")
    left, right = lax.rem(gx + nx - 1, nx), lax.rem(gx + 1, nx)
    down, up = lax.rem(gz + nz - 1, nz), lax.rem(gz + 1, nz)
    has_left, has_right = gx > 0, gx < nx - 1
    has_down, has_up = gz > 0, gz < nz - 1
    ny = flow.shape[-1]
    levels_total = nl * nz
    depth, rows = S0.shape[1], S0.shape[2]
    if nz == 2:
        base = 1 + ZH * gz
        base_up, base_down = 1 + ZH, 1

        def span(h):
            return base - h * gz, nl + h
    else:
        base = base_up = base_down = 1 + ZH

        def span(h):
            return base - h, nl + 2 * h

    own = pl.ds(base, nl)
    mine = slice(PAD, PAD + nxl)
    lo, hi = PAD - 8, PAD + nxl + 8
    c, m, p = slice(lo, hi), slice(lo - 1, hi - 1), slice(lo + 1, hi + 1)
    width = hi - lo

    copies = [
        pltpu.make_async_copy(flow, S0.at[pl.ds(0, 4), own, mine], loc.at[0]),
        pltpu.make_async_copy(fluid, S0.at[4, own, mine], loc.at[1]),
        pltpu.make_async_copy(thickness, G.at[0, mine], loc.at[2]),
        pltpu.make_async_copy(bed, G.at[1, mine], loc.at[3]),
        pltpu.make_async_copy(mask, M.at[mine], loc.at[4]),
        pltpu.make_async_copy(density, DN, loc.at[5]),
        pltpu.make_async_copy(smb, SM, loc.at[6]),
    ]
    for copy in copies:
        copy.start()

    barrier = pltpu.get_barrier_semaphore()

    @pl.when(has_left)
    def _():
        pl.semaphore_signal(barrier, inc=1, device_id={"gx": left}, device_id_type=MESH)

    @pl.when(has_right)
    def _():
        pl.semaphore_signal(barrier, inc=1, device_id={"gx": right}, device_id_type=MESH)

    for off in range(1, nz):
        pl.semaphore_signal(barrier, inc=1, device_id={"gz": lax.rem(gz + off, nz)}, device_id_type=MESH)

    zrow = jnp.zeros((rows, ny), jnp.float32)
    for k in (0, depth - 1):
        for f in range(4):
            S0[f, k] = zrow
            S1[f, k] = zrow
        for f in range(3):
            T[f, k] = zrow

    def outside_x(where):
        strip = slice(PAD - 8, PAD) if where == 0 else slice(PAD + nxl, PAD + nxl + 8)
        zero = jnp.zeros((8, ny), jnp.float32)

        def one(k, _):
            for f in range(4):
                S0[f, k, strip] = zero
            S0[4, k, strip] = zero + 1.0
            return 0

        lax.fori_loop(1, depth - 1, one, 0)
        G[0, strip] = zero
        G[1, strip] = zero
        M[strip] = jnp.zeros((8, ny), jnp.int32)

    @pl.when(jnp.logical_not(has_left))
    def _():
        outside_x(0)

    @pl.when(jnp.logical_not(has_right))
    def _():
        outside_x(1)

    if nz > 2:
        def outside_z(start):
            for k in range(start, start + ZH):
                for f in range(4):
                    S0[f, k, c] = jnp.zeros((width, ny), jnp.float32)
                S0[4, k, c] = jnp.ones((width, ny), jnp.float32)

        @pl.when(jnp.logical_not(has_down))
        def _():
            outside_z(1)

        @pl.when(jnp.logical_not(has_up))
        def _():
            outside_z(1 + ZH + nl)

    def remote(src, dst, number, device):
        return pltpu.make_async_remote_copy(src_ref=src, dst_ref=dst, send_sem=send.at[number],
                                            recv_sem=recv.at[number], device_id=device, device_id_type=MESH)

    first, last = pl.ds(PAD, XH), pl.ds(PAD + nxl - XH, XH)
    from_left, from_right = pl.ds(PAD - XH, XH), pl.ds(PAD + nxl, XH)
    every = pl.ds(0, 5)
    leftward = [
        remote(S0.at[every, own, first], S0.at[every, own, from_right], 0, {"gx": left}),
        remote(G.at[:, first], G.at[:, from_right], 1, {"gx": left}),
        remote(M.at[first], M.at[from_right], 2, {"gx": left}),
    ]
    rightward = [
        remote(S0.at[every, own, last], S0.at[every, own, from_left], 3, {"gx": right}),
        remote(G.at[:, last], G.at[:, from_left], 4, {"gx": right}),
        remote(M.at[last], M.at[from_left], 5, {"gx": right}),
    ]
    top, bottom = pl.ds(base + nl - ZH, ZH), pl.ds(base, ZH)
    from_down, from_up = pl.ds(base_up - ZH, ZH), pl.ds(base_down + nl, ZH)
    pieces = (pl.ds(PAD, nxl), from_left, from_right)
    upward = [remote(S0.at[every, top, piece], S0.at[every, from_down, piece], 6 + n, {"gz": up})
              for n, piece in enumerate(pieces)]
    downward = [remote(S0.at[every, bottom, piece], S0.at[every, from_up, piece], 9 + n, {"gz": down})
                for n, piece in enumerate(pieces)]

    for n in range(5):
        copies[n].wait()
    pl.semaphore_wait(barrier, nz - 1 + jnp.where(has_left, 1, 0) + jnp.where(has_right, 1, 0))

    @pl.when(has_left)
    def _():
        for copy in leftward:
            copy.start()

    @pl.when(has_right)
    def _():
        for copy in rightward:
            copy.start()

    @pl.when(has_up)
    def _():
        upward[0].start()

    @pl.when(has_down)
    def _():
        downward[0].start()

    copies[5].wait()
    copies[6].wait()
    total = jnp.zeros((nxl, ny), jnp.float32)
    for k in reversed(range(nl)):
        cell = DN[k]
        DN[k] = total + 0.5 * cell
        total = total + cell
    FS[2, mine] = total

    def dy(f):
        axis = f.ndim - 1
        lane = lax.broadcasted_iota(jnp.int32, f.shape, axis)
        return (jnp.where(lane < ny - 1, pltpu.roll(f, ny - 1, axis), 0.0)
                - jnp.where(lane > 0, pltpu.roll(f, 1, axis), 0.0))

    def inside(start, height):
        column = gx * nxl + lax.broadcasted_iota(jnp.int32, (height, ny), 0) + (start - PAD)
        return (column >= 0) & (column < nx * nxl)

    def plan(start, height):
        c = slice(start, start + height)
        A[0, c] = 0.5 * (FX[start + 1:start + height + 1] - FX[start - 1:start + height - 1])
        A[1, c] = 0.5 * dy(FX[c])
        A[2, c] = jnp.where(inside(start, height) & (M[c] > 0), 1.0, 0.0)
        A[3, c] = jnp.where(M[c] == 1, FRICTION, 0.0)

    def level_at(k, count):
        return gz * nl + k - base + lax.broadcasted_iota(jnp.int32, (count, 1, ny), 0)

    def stress(B, k, count, start, height):
        at = pl.ds(k, count)
        c = slice(start, start + height)
        m, p = slice(start - 1, start + height - 1), slice(start + 1, start + height + 1)
        above, below = pl.ds(k + 1, count), pl.ds(k - 1, count)
        xx, vx, wx = (B[f, at, p] - B[f, at, m] for f in range(3))
        uz, vz, zz = (B[f, above, c] - B[f, below, c] for f in range(3))
        uy, yy, wy = (dy(B[f, at, c]) for f in range(3))
        xy, xz, yz = uy + vx, uz + wx, vz + wy
        twice = xx * xx + yy * yy + zz * zz
        second = 0.0625 * (twice + twice + (xy * xy + xz * xz + yz * yz))
        third = jnp.log2(S0[4, at, c] * (second + REGULAR)) * (1.0 / 3.0)
        a = jnp.exp2(-third)
        V[0, at, c] = (2.0 * STEP) * jnp.exp2(third)
        V[1, at, c] = (0.25 * STEP) * a * (xx + yy + zz)
        h = 0.25 * a
        if height == 8:
            h = jnp.where(jnp.broadcast_to(inside(start, height)[None], h.shape), h, 0.0)
        if nz > 2:
            level = level_at(k, count)
            ok = jnp.where((level >= 0) & (level < levels_total), 1.0, 0.0)
            h = jnp.where(jnp.broadcast_to(ok, h.shape) > 0.0, h, 0.0)
        g = 0.5 * h
        T[0, at, c] = g * xz
        T[1, at, c] = g * yz
        T[2, at, c] = h * zz
        T[3, at, c] = h * xx
        T[4, at, c] = g * xy
        T[5, at, c] = h * yy

    def move(B, k, count, start, height):
        at = pl.ds(k, count)
        c = slice(start, start + height)
        m, p = slice(start - 1, start + height - 1), slice(start + 1, start + height + 1)
        above, below = pl.ds(k + 1, count), pl.ds(k - 1, count)
        level = level_at(k, count)
        drag = jnp.where(level == 0, 1.0, 0.0) * A[3, c][None]
        u, v, press = B[0, at, c], B[1, at, c], B[3, at, c]
        fx = ((T[3, at, p] - T[3, at, m]) + dy(T[4, at, c]) + (T[0, above, c] - T[0, below, c])
              - 0.5 * (B[3, at, p] - B[3, at, m]) - A[0, c][None] - drag * u)
        fy = ((T[4, at, p] - T[4, at, m]) + dy(T[5, at, c]) + (T[1, above, c] - T[1, below, c])
              - 0.5 * dy(press) - A[1, c][None] - drag * v)
        fz = ((T[0, at, p] - T[0, at, m]) + dy(T[1, at, c]) + (T[2, above, c] - T[2, below, c])
              - 0.5 * (B[3, above, c] - B[3, below, c]))
        step = V[0, at, c]
        ice = jnp.broadcast_to(A[2, c][None], u.shape)
        if nz > 2:
            ice = ice * jnp.where((level >= 0) & (level < levels_total), 1.0, 0.0)
        return [jnp.where(ice > 0.0, value, 0.0) for value in (
            u + step * fx, v + step * fy, B[2, at, c] + step * fz, press - V[1, at, c])]

    def blocks(reach, most, step, areas):
        start, count = span(reach)
        pieces = -(-count // most)
        for n in range(pieces):
            one, two = count * n // pieces, count * (n + 1) // pieces
            for area in areas:
                step(start + one, two - one, *area)

    def stress_first(*at):
        stress(S0, *at)

    def stress_last(*at):
        stress(S1, *at)

    def move_first(k, count, start, height):
        for f, value in enumerate(move(S0, k, count, start, height)):
            S1[f, pl.ds(k, count), start:start + height] = value

    def move_last(k, count, start, height):
        for f, value in enumerate(move(S1, k, count, start, height)):
            flow_out[f, pl.ds(k - base, count), start:start + height] = value

    middle = [(PAD + 1, nxl - 2)]
    FX[mine] = G[1, mine] + G[0, mine]
    plan(*middle[0])
    for flag, group in ((has_down, upward), (has_up, downward)):
        @pl.when(flag)
        def _():
            group[0].wait_recv()

    blocks(3, 2, stress_first, middle)
    blocks(2, 2, move_first, middle)
    blocks(1, 2, stress_last, middle)

    @pl.when(has_left)
    def _():
        for copy in rightward:
            copy.wait_recv()

    @pl.when(has_left & has_up)
    def _():
        upward[1].start()

    @pl.when(has_left & has_down)
    def _():
        downward[1].start()

    @pl.when(has_right)
    def _():
        for copy in leftward:
            copy.wait_recv()

    @pl.when(has_right & has_up)
    def _():
        upward[2].start()

    @pl.when(has_right & has_down)
    def _():
        downward[2].start()

    blocks(0, 2, move_last, middle)

    ends = [(PAD - 4, 8), (PAD + nxl - 4, 8)]
    for start in (PAD - 8, PAD + nxl):
        strip = slice(start, start + 8)
        FX[strip] = G[1, strip] + G[0, strip]
    for area in ends:
        plan(*area)
    for flag, group in ((has_down, upward), (has_up, downward)):
        @pl.when(flag & has_left)
        def _():
            group[1].wait_recv()

        @pl.when(flag & has_right)
        def _():
            group[2].wait_recv()

    blocks(3, 6, stress_first, ends)
    blocks(2, 6, move_first, [(PAD - 5, 8), (PAD + nxl - 3, 8)])
    blocks(1, 6, stress_last, ends)
    blocks(0, 4, move_last, ends)
    sum_u, sum_v = flow_out[0, 0, c], flow_out[1, 0, c]
    for k in range(1, nl):
        sum_u = sum_u + flow_out[0, k, c]
        sum_v = sum_v + flow_out[1, k, c]
    FS[0, c] = sum_u
    FS[1, c] = sum_v

    sums = [pltpu.make_async_remote_copy(
        src_ref=FS.at[:, pl.ds(lo, width)], dst_ref=FR.at[off - 1, :, pl.ds(lo, width)],
        send_sem=fsend.at[off - 1], recv_sem=frecv.at[off - 1],
        device_id={"gz": lax.rem(gz + off, nz)}, device_id_type=MESH) for off in range(1, nz)]
    for copy in sums:
        copy.start()
    above = jnp.zeros((nxl, ny), jnp.float32)
    for off in range(1, nz):
        sums[off - 1].wait_recv()
        sum_u = sum_u + FR[off - 1, 0, c]
        sum_v = sum_v + FR[off - 1, 1, c]
        above = above + jnp.where(gz < off, 1.0, 0.0) * FR[off - 1, 2, mine]
    part = G[0, c] * (1.0 / levels_total)
    FX[c] = part * sum_u
    flux_y = dy(part * sum_v)[8:8 + nxl]
    spread = FX[PAD + 1:PAD + nxl + 1] - FX[PAD - 1:PAD + nxl - 1] + flux_y
    fresh = G[0, mine] + TIME_STEP * (SM[...] - 0.5 * spread)
    new_thickness[...] = fresh
    weight = fresh * (1.0 / levels_total)
    for k in range(nl):
        overburden[k] = weight * (above + DN[k])

    @pl.when(has_left)
    def _():
        for copy in leftward:
            copy.wait_send()

    @pl.when(has_right)
    def _():
        for copy in rightward:
            copy.wait_send()

    for flag, group in ((has_up, upward), (has_down, downward)):
        @pl.when(flag)
        def _():
            group[0].wait_send()

        @pl.when(flag & has_left)
        def _():
            group[1].wait_send()

        @pl.when(flag & has_right)
        def _():
            group[2].wait_send()

    for copy in sums:
        copy.wait_send()


def paired(nx, nl, nxl, flow, fluid, density, thickness, bed, smb, mask,
           flow_out, new_thickness, overburden,
           S0, S1, T, V, G, M, PK, RK, SM, DN, A, FX, FM, RM, FE, RE, FD, RD,
           loc, send, recv):
    gx, gz = lax.axis_index("gx"), lax.axis_index("gz")
    left, right = lax.rem(gx + nx - 1, nx), lax.rem(gx + 1, nx)
    has_left, has_right = gx > 0, gx < nx - 1
    odd = lax.rem(gx, 2)
    near = gx + 1 - 2 * odd
    far = lax.rem(gx + nx - 1 + 2 * odd, nx)
    has_far = jnp.where(odd == 1, gx, nx - 1 - gx) < nx - 1
    ny = flow.shape[-1]
    levels_total = 2 * nl
    depth, rows = S0.shape[1], S0.shape[2]
    base = 1 + ZH * gz
    own = pl.ds(base, nl)
    facing = pl.ds(1 + nl - ZH + gz * (2 * ZH - nl), ZH)
    others = pl.ds(1 + gz * 2 * ZH, nl - ZH)
    across = pl.ds(1 + gz * nl, ZH)
    mine = slice(PAD, PAD + nxl)

    barrier = pltpu.get_barrier_semaphore()
    pl.semaphore_signal(barrier, inc=1, device_id={"gx": near}, device_id_type=MESH)
    pl.semaphore_signal(barrier, inc=1, device_id={"gz": 1 - gz}, device_id_type=MESH)

    @pl.when(has_far)
    def _():
        pl.semaphore_signal(barrier, inc=1, device_id={"gx": far}, device_id_type=MESH)

    copies = [
        pltpu.make_async_copy(flow, S0.at[pl.ds(0, 4), own, mine], loc.at[0]),
        pltpu.make_async_copy(fluid, S0.at[4, own, mine], loc.at[1]),
        pltpu.make_async_copy(thickness, G.at[0, mine], loc.at[2]),
        pltpu.make_async_copy(bed, G.at[1, mine], loc.at[3]),
        pltpu.make_async_copy(mask, M, loc.at[4]),
        pltpu.make_async_copy(density, DN, loc.at[5]),
        pltpu.make_async_copy(smb, SM, loc.at[6]),
    ]
    for copy in copies:
        copy.start()

    zrow = jnp.zeros((rows, ny), jnp.float32)
    for k in (0, depth - 1):
        for f in range(4):
            S0[f, k] = zrow
            S1[f, k] = zrow
        for f in range(3):
            T[f, k] = zrow

    def outside_x(where):
        strip = slice(PAD - 8, PAD) if where == 0 else slice(PAD + nxl, PAD + nxl + 8)
        zero = jnp.zeros((8, ny), jnp.float32)

        def one(k, _):
            for f in range(4):
                S0[f, k, strip] = zero
            S0[4, k, strip] = zero + 1.0
            return 0

        lax.fori_loop(1, depth - 1, one, 0)
        G[0, strip] = zero
        G[2, strip] = zero
        FX[strip] = zero

    @pl.when(jnp.logical_not(has_left))
    def _():
        outside_x(0)

    @pl.when(jnp.logical_not(has_right))
    def _():
        outside_x(1)

    def remote(src, dst, number, device):
        return pltpu.make_async_remote_copy(src_ref=src, dst_ref=dst, send_sem=send.at[number],
                                            recv_sem=recv.at[number], device_id=device, device_id_type=MESH)

    motion, state = pl.ds(0, 3), pl.ds(3, 2)

    def halo(levels, src, dst, number, device):
        (src_uvw, src_pf), (dst_uvw, dst_pf) = src, dst
        return [remote(S0.at[motion, levels, src_uvw], S0.at[motion, levels, dst_uvw], number, device),
                remote(S0.at[state, levels, src_pf], S0.at[state, levels, dst_pf], number + 1, device)]

    first = pl.ds(PAD, XH), pl.ds(PAD, XH - 1)
    last = pl.ds(PAD + nxl - XH, XH), pl.ds(PAD + nxl - XH + 1, XH - 1)
    from_left = pl.ds(PAD - XH, XH), pl.ds(PAD - XH + 1, XH - 1)
    from_right = pl.ds(PAD + nxl, XH), pl.ds(PAD + nxl, XH - 1)

    def sideways(src, dst, side, number, device):
        early = halo(facing, src, dst, number, device)
        early.append(remote(PK.at[side], RK.at[1 - side], number + 2, device))
        return early, halo(others, src, dst, number + 3, device)

    leftward = sideways(first, from_right, 0, 0, {"gx": left})
    rightward = sideways(last, from_left, 1, 5, {"gx": right})
    partner = {"gz": 1 - gz}
    planes = remote(S0.at[pl.ds(0, 5), facing, pl.ds(PAD, nxl)], S0.at[pl.ds(0, 5), across, pl.ds(PAD, nxl)], 10, partner)

    def corner(at, number):
        (uvw, pf) = at
        return [remote(S0.at[motion, facing, uvw], S0.at[motion, across, uvw], number, partner),
                remote(S0.at[state, facing, pf], S0.at[state, across, pf], number + 1, partner)]

    corners = corner(from_left, 11), corner(from_right, 13)
    weights = remote(FD, RD, 15, partner)
    inner = remote(FM, RM, 16, partner)
    strips = [remote(FE.at[side], RE.at[side], 17 + side, partner) for side in range(2)]
    incoming = rightward, leftward
    have = (has_left, has_right)

    for n in range(5):
        copies[n].wait()
    G[2, mine] = M[...].astype(jnp.float32)
    FX[mine] = G[1, mine] + G[0, mine]
    end = PAD + nxl
    PK[0, 0:4] = FX[PAD:PAD + 4]
    PK[0, 4:7] = G[2, PAD:PAD + 3]
    PK[0, 7:8] = G[0, PAD:PAD + 1]
    PK[1, 0:4] = FX[end - 4:end]
    PK[1, 4:7] = G[2, end - 3:end]
    PK[1, 7:8] = G[0, end - 1:end]

    pl.semaphore_wait(barrier, 2 + jnp.where(has_far, 1, 0))

    def launch(group, flag):
        @pl.when(flag)
        def _():
            for copy in group:
                copy.start()

    launch(leftward[0], odd == 1)
    launch(rightward[0], odd == 0)
    eager = lax.rem(gx + 1, 4) < 2
    launch(leftward[1], (odd == 1) & eager)
    launch(rightward[1], (odd == 0) & eager)
    planes.start()

    launch(rightward[0], (odd == 1) & has_right)
    launch(leftward[0], (odd == 0) & has_left & jnp.logical_not(eager))
    launch(leftward[1], (odd == 1) & jnp.logical_not(eager))
    launch(rightward[1], (odd == 0) & jnp.logical_not(eager))
    launch(rightward[1], (odd == 1) & has_right)
    launch(leftward[1], (odd == 0) & has_left & jnp.logical_not(eager))


    def dy(f):
        axis = f.ndim - 1
        lane = lax.broadcasted_iota(jnp.int32, f.shape, axis)
        return (jnp.where(lane < ny - 1, pltpu.roll(f, ny - 1, axis), 0.0)
                - jnp.where(lane > 0, pltpu.roll(f, 1, axis), 0.0))

    def inside(start, height):
        column = gx * nxl + lax.broadcasted_iota(jnp.int32, (height, ny), 0) + (start - PAD)
        return (column >= 0) & (column < nx * nxl)

    def plan(start, height):
        c = slice(start, start + height)
        A[0, c] = 0.5 * (FX[start + 1:start + height + 1] - FX[start - 1:start + height - 1])
        A[1, c] = 0.5 * dy(FX[c])
        A[2, c] = jnp.where(inside(start, height) & (G[2, c] > 0.0), 1.0, 0.0)
        A[3, c] = jnp.where(G[2, c] == 1.0, FRICTION, 0.0)

    def level_at(k, count):
        return gz * nl + k - base + lax.broadcasted_iota(jnp.int32, (count, 1, ny), 0)

    def stress(B, k, count, start, height):
        at = pl.ds(k, count)
        c = slice(start, start + height)
        m, p = slice(start - 1, start + height - 1), slice(start + 1, start + height + 1)
        above, below = pl.ds(k + 1, count), pl.ds(k - 1, count)
        xx, vx, wx = (B[f, at, p] - B[f, at, m] for f in range(3))
        uz, vz, zz = (B[f, above, c] - B[f, below, c] for f in range(3))
        uy, yy, wy = (dy(B[f, at, c]) for f in range(3))
        xy, xz, yz = uy + vx, uz + wx, vz + wy
        twice = xx * xx + yy * yy + zz * zz
        second = 0.0625 * (twice + twice + (xy * xy + xz * xz + yz * yz))
        third = jnp.log2(S0[4, at, c] * (second + REGULAR)) * (1.0 / 3.0)
        a = jnp.exp2(-third)
        V[0, at, c] = (2.0 * STEP) * jnp.exp2(third)
        V[1, at, c] = (0.25 * STEP) * a * (xx + yy + zz)
        h = 0.25 * a
        if height == 8:
            h = jnp.where(jnp.broadcast_to(inside(start, height)[None], h.shape), h, 0.0)
        g = 0.5 * h
        q = 0.5 * B[3, at, c]
        T[0, at, c] = g * xz
        T[1, at, c] = g * yz
        T[2, at, c] = h * zz - q
        T[3, at, c] = h * xx - q
        T[4, at, c] = g * xy
        T[5, at, c] = h * yy - q

    def move(B, k, count, start, height):
        at = pl.ds(k, count)
        c = slice(start, start + height)
        m, p = slice(start - 1, start + height - 1), slice(start + 1, start + height + 1)
        above, below = pl.ds(k + 1, count), pl.ds(k - 1, count)
        drag = jnp.where(level_at(k, count) == 0, 1.0, 0.0) * A[3, c][None]
        u, v, press = B[0, at, c], B[1, at, c], B[3, at, c]
        fx = ((T[3, at, p] - T[3, at, m]) + dy(T[4, at, c]) + (T[0, above, c] - T[0, below, c])
              - A[0, c][None] - drag * u)
        fy = ((T[4, at, p] - T[4, at, m]) + dy(T[5, at, c]) + (T[1, above, c] - T[1, below, c])
              - A[1, c][None] - drag * v)
        fz = ((T[0, at, p] - T[0, at, m]) + dy(T[1, at, c]) + (T[2, above, c] - T[2, below, c]))
        step = V[0, at, c]
        ice = jnp.broadcast_to(A[2, c][None], u.shape)
        return [jnp.where(ice > 0.0, value, 0.0) for value in (
            u + step * fx, v + step * fy, B[2, at, c] + step * fz, press - V[1, at, c])]

    def blocks(start, count, most, step, area):
        pieces = -(-count // most)
        for n in range(pieces):
            one, two = count * n // pieces, count * (n + 1) // pieces
            step(start + one, two - one, *area)

    def apart(reach, most, step, area):
        blocks(1 + gz * (2 * ZH - reach), nl - ZH + reach, most, step, area)

    def facing_part(reach, most, step, area):
        low, high = 1 + nl - ZH + reach, 1 + ZH - reach
        blocks(low + gz * (high - low), ZH, most, step, area)

    def reached(reach, most, step, area):
        low = 1 + nl - reach
        blocks(low + gz * (1 + ZH - reach - low), 2 * (ZH - 4 + reach), most, step, area)

    def rest(reach, most, step, area):
        count = nl - reach
        blocks(1 + gz * (ZH + nl - count), count, most, step, area)

    def stress_first(*at):
        stress(S0, *at)

    def stress_last(*at):
        stress(S1, *at)

    def move_first(k, count, start, height):
        for f, value in enumerate(move(S0, k, count, start, height)):
            S1[f, pl.ds(k, count), start:start + height] = value

    def move_last(k, count, start, height):
        for f, value in enumerate(move(S1, k, count, start, height)):
            flow_out[f, pl.ds(k - base, count), start:start + height] = value

    middle = (PAD + 1, nxl - 2)
    plan(*middle)
    apart(3, 2, stress_first, middle)

    copies[5].wait()
    copies[6].wait()
    total = jnp.zeros((nxl, ny), jnp.float32)
    for k in reversed(range(nl)):
        cell = DN[k]
        DN[k] = total + 0.5 * cell
        total = total + cell
    FD[...] = total
    weights.start()

    apart(2, 2, move_first, middle)
    launch(leftward[0], (odd == 0) & has_left & eager)
    launch(leftward[1], (odd == 0) & has_left & eager)
    apart(1, 2, stress_last, middle)
    apart(0, 2, move_last, middle)
    planes.wait_recv()
    facing_part(3, 2, stress_first, middle)

    def forward(side):
        @pl.when(have[side])
        def _():
            for copy in incoming[side][0][:2]:
                copy.wait_recv()
            for copy in corners[side]:
                copy.start()

    left_leads = (gx == 0) | ((odd == 1) & has_right)

    def by_arrival(step):
        @pl.when(left_leads)
        def _():
            step(0, 1)

        @pl.when(jnp.logical_not(left_leads))
        def _():
            step(1, 0)

    facing_part(2, 2, move_first, middle)
    facing_part(1, 2, stress_last, middle)
    facing_part(0, 2, move_last, middle)

    by_arrival(lambda lead, other: forward(lead))

    def depth_sum(f, c):
        value = flow_out[f, 0, c]
        for k in range(1, nl):
            value = value + flow_out[f, k, c]
        return value

    for f in range(2):
        FM[f] = depth_sum(f, mine)
    inner.start()

    edges = [((PAD - 4, 8), (PAD - 5, 8)), ((PAD + nxl - 4, 8), (PAD + nxl - 3, 8))]

    def approach(side):
        area, shifted = edges[side]

        @pl.when(have[side])
        def _():
            incoming[side][0][2].wait_recv()
            at = PAD if side == 0 else end
            for row in range(4):
                to = at - 4 + row if side == 0 else at + row
                FX[to:to + 1] = RK[side, row:row + 1]
            for row in range(3):
                to = at - 3 + row if side == 0 else at + row
                G[2, to:to + 1] = RK[side, 4 + row:5 + row]
            to = at - 1 if side == 0 else at
            G[0, to:to + 1] = RK[side, 7:8]
            for copy in corners[side]:
                copy.wait_recv()

        plan(*area)
        reached(3, 3, stress_first, area)
        reached(2, 4, move_first, shifted)
        reached(1, 4, stress_last, area)

    def finish(side):
        area, shifted = edges[side]

        @pl.when(have[side])
        def _():
            for copy in incoming[side][1]:
                copy.wait_recv()

        rest(3, 5, stress_first, area)
        rest(2, 6, move_first, shifted)
        rest(1, 4, stress_last, area)
        rest(0, 4, move_last, area)
        wide = slice(PAD - 8, PAD + 8) if side == 0 else slice(PAD + nxl - 8, PAD + nxl + 8)
        for f in range(2):
            FE[side, f] = depth_sum(f, wide)
        strips[side].start()

    def both(lead, other):
        forward(other)
        approach(lead)
        finish(lead)
        approach(other)
        finish(other)

    by_arrival(both)

    def settle(start, height, sum_v):
        c = slice(start, start + height)
        o = slice(start - PAD, start - PAD + height)
        flux_y = dy(G[0, c] * (1.0 / levels_total) * sum_v)
        spread = FX[start + 1:start + height + 1] - FX[start - 1:start + height - 1] + flux_y
        fresh = G[0, c] + TIME_STEP * (SM[o] - 0.5 * spread)
        new_thickness[o] = fresh
        weight = fresh * (1.0 / levels_total)
        above = jnp.where(gz == 0, 1.0, 0.0) * RD[o]
        for k in range(nl):
            overburden[k, o] = weight * (above + DN[k, o])

    weights.wait_recv()
    inner.wait_recv()
    FX[mine] = G[0, mine] * (1.0 / levels_total) * (FM[0] + RM[0])
    settle(PAD + 8, nxl - 16, FM[1, 8:nxl - 8] + RM[1, 8:nxl - 8])
    def conclude(side):
        strips[side].wait_recv()
        begin = PAD - 8 if side == 0 else PAD + nxl - 8
        wide = slice(begin, begin + 16)
        FX[wide] = G[0, wide] * (1.0 / levels_total) * (FE[side, 0] + RE[side, 0])
        inward = slice(8, 16) if side == 0 else slice(0, 8)
        settle(PAD if side == 0 else PAD + nxl - 8, 8, FE[side, 1, inward] + RE[side, 1, inward])

    def close(lead, other):
        conclude(lead)
        conclude(other)

    by_arrival(close)

    for side, group in ((0, leftward), (1, rightward)):
        @pl.when(have[side])
        def _():
            for copy in (*group[0], *group[1], *corners[side]):
                copy.wait_send()

    for copy in (planes, weights, inner, *strips):
        copy.wait_send()


def write(nxl, held, fresh, weight, flow_out, new_thickness, overburden, done):
    copies = [
        pltpu.make_async_copy(held.at[:, :, pl.ds(PAD, nxl)], flow_out, done.at[0]),
        pltpu.make_async_copy(fresh, new_thickness, done.at[1]),
        pltpu.make_async_copy(weight, overburden, done.at[2]),
    ]
    for copy in copies:
        copy.start()
    for copy in copies:
        copy.wait()


def solution(mesh):
    nx, nz = mesh.shape["gx"], mesh.shape["gz"]

    def body(flow, fluid, density, thickness, bed, smb, mask):
        nl, nxl, ny = fluid.shape
        depth = nl + 2 + (ZH if nz == 2 else 2 * ZH)
        rows = nxl + 2 * PAD
        f32 = jnp.float32
        vmem = pl.BlockSpec(memory_space=pltpu.VMEM)
        block = [pltpu.VMEM((n, depth, rows, ny), f32) for n in (5, 4, 6, 2)]
        if nz == 2 and nx % 2 == 0 and nl > ZH and nxl >= 24:
            body_of = functools.partial(paired, nx, nl, nxl)
            scratch = block + [
                pltpu.VMEM((3, rows, ny), f32),
                pltpu.VMEM((nxl, ny), jnp.int32),
                pltpu.VMEM((2, 8, ny), f32),
                pltpu.VMEM((2, 8, ny), f32),
                pltpu.VMEM((nxl, ny), f32),
                pltpu.VMEM((nl, nxl, ny), f32),
                pltpu.VMEM((4, rows, ny), f32),
                pltpu.VMEM((rows, ny), f32),
                pltpu.VMEM((2, nxl, ny), f32),
                pltpu.VMEM((2, nxl, ny), f32),
                pltpu.VMEM((2, 2, 16, ny), f32),
                pltpu.VMEM((2, 2, 16, ny), f32),
                pltpu.VMEM((nxl, ny), f32),
                pltpu.VMEM((nxl, ny), f32),
                pltpu.SemaphoreType.DMA((7,)),
                pltpu.SemaphoreType.DMA((19,)),
                pltpu.SemaphoreType.DMA((19,)),
            ]
        else:
            body_of = functools.partial(kernel, nx, nz, nl, nxl)
            scratch = block + [
                pltpu.VMEM((2, rows, ny), f32),
                pltpu.VMEM((rows, ny), jnp.int32),
                pltpu.VMEM((nxl, ny), f32),
                pltpu.VMEM((nl, nxl, ny), f32),
                pltpu.VMEM((4, rows, ny), f32),
                pltpu.VMEM((rows, ny), f32),
                pltpu.VMEM((3, rows, ny), f32),
                pltpu.VMEM((nz - 1, 3, rows, ny), f32),
                pltpu.SemaphoreType.DMA((7,)),
                pltpu.SemaphoreType.DMA((12,)),
                pltpu.SemaphoreType.DMA((12,)),
                pltpu.SemaphoreType.DMA((nz - 1,)),
                pltpu.SemaphoreType.DMA((nz - 1,)),
            ]
        held, fresh, weight = pl.pallas_call(
            body_of,
            out_shape=(
                pltpu.VMEM((4, nl, rows, ny), f32),
                pltpu.VMEM(thickness.shape, f32),
                pltpu.VMEM(density.shape, f32),
            ),
            in_specs=[pl.BlockSpec(memory_space=pl.ANY)] * 7,
            out_specs=(vmem, vmem, vmem),
            scratch_shapes=scratch,
            compiler_params=pltpu.CompilerParams(collective_id=0, has_side_effects=True),
        )(flow, fluid, density, thickness, bed, smb, mask)
        anywhere = pl.BlockSpec(memory_space=pl.ANY)
        return pl.pallas_call(
            functools.partial(write, nxl),
            out_shape=(
                jax.ShapeDtypeStruct(flow.shape, f32),
                jax.ShapeDtypeStruct(thickness.shape, f32),
                jax.ShapeDtypeStruct(density.shape, f32),
            ),
            in_specs=[vmem] * 3,
            out_specs=(anywhere,) * 3,
            scratch_shapes=[pltpu.SemaphoreType.DMA((3,))],
        )(*(pltpu.with_memory_space_constraint(x, pltpu.VMEM) for x in (held, fresh, weight)))

    placed = (
        P(None, "gz", "gx", None), P("gz", "gx", None), P("gz", "gx", None),
        P("gx", None), P("gx", None), P("gx", None), P("gx", None),
    )
    return jax.shard_map(
        body, mesh=mesh, in_specs=placed,
        out_specs=(P(None, "gz", "gx", None), P("gx", None), P("gz", "gx", None)),
        check_vma=False,
    )
```

```python
import functools

import jax
import jax.numpy as jnp
from jax import lax
from jax.experimental import pallas as pl
from jax.experimental.pallas import tpu as pltpu
from jax.sharding import PartitionSpec as P

REGULAR = 0.01
FRICTION = 2.0
STEP = 0.2
TIME_STEP = 0.5

XH = 5
ZH = 4
PAD = 16
MESH = pl.DeviceIdType.MESH


def kernel(nx, nz, nl, nxl, flow, fluid, density, thickness, bed, smb, mask,
           flow_out, new_thickness, overburden,
           S0, S1, T, V, G, M, SM, DN, A, FX, FS, FR,
           loc, send, recv, fsend, frecv):
    gx, gz = lax.axis_index("gx"), lax.axis_index("gz")
    left, right = lax.rem(gx + nx - 1, nx), lax.rem(gx + 1, nx)
    down, up = lax.rem(gz + nz - 1, nz), lax.rem(gz + 1, nz)
    has_left, has_right = gx > 0, gx < nx - 1
    has_down, has_up = gz > 0, gz < nz - 1
    ny = flow.shape[-1]
    levels_total = nl * nz
    depth, rows = S0.shape[1], S0.shape[2]
    if nz == 2:
        base = 1 + ZH * gz
        base_up, base_down = 1 + ZH, 1

        def span(h):
            return base - h * gz, nl + h
    else:
        base = base_up = base_down = 1 + ZH

        def span(h):
            return base - h, nl + 2 * h

    own = pl.ds(base, nl)
    mine = slice(PAD, PAD + nxl)
    lo, hi = PAD - 8, PAD + nxl + 8
    c, m, p = slice(lo, hi), slice(lo - 1, hi - 1), slice(lo + 1, hi + 1)
    width = hi - lo

    copies = [
        pltpu.make_async_copy(flow, S0.at[pl.ds(0, 4), own, mine], loc.at[0]),
        pltpu.make_async_copy(fluid, S0.at[4, own, mine], loc.at[1]),
        pltpu.make_async_copy(thickness, G.at[0, mine], loc.at[2]),
        pltpu.make_async_copy(bed, G.at[1, mine], loc.at[3]),
        pltpu.make_async_copy(mask, M.at[mine], loc.at[4]),
        pltpu.make_async_copy(density, DN, loc.at[5]),
        pltpu.make_async_copy(smb, SM, loc.at[6]),
    ]
    for copy in copies:
        copy.start()

    barrier = pltpu.get_barrier_semaphore()

    @pl.when(has_left)
    def _():
        pl.semaphore_signal(barrier, inc=1, device_id={"gx": left}, device_id_type=MESH)

    @pl.when(has_right)
    def _():
        pl.semaphore_signal(barrier, inc=1, device_id={"gx": right}, device_id_type=MESH)

    for off in range(1, nz):
        pl.semaphore_signal(barrier, inc=1, device_id={"gz": lax.rem(gz + off, nz)}, device_id_type=MESH)

    zrow = jnp.zeros((rows, ny), jnp.float32)
    for k in (0, depth - 1):
        for f in range(4):
            S0[f, k] = zrow
            S1[f, k] = zrow
        for f in range(3):
            T[f, k] = zrow

    def outside_x(where):
        strip = slice(PAD - 8, PAD) if where == 0 else slice(PAD + nxl, PAD + nxl + 8)
        zero = jnp.zeros((8, ny), jnp.float32)

        def one(k, _):
            for f in range(4):
                S0[f, k, strip] = zero
            S0[4, k, strip] = zero + 1.0
            return 0

        lax.fori_loop(1, depth - 1, one, 0)
        G[0, strip] = zero
        G[1, strip] = zero
        M[strip] = jnp.zeros((8, ny), jnp.int32)

    @pl.when(jnp.logical_not(has_left))
    def _():
        outside_x(0)

    @pl.when(jnp.logical_not(has_right))
    def _():
        outside_x(1)

    if nz > 2:
        def outside_z(start):
            for k in range(start, start + ZH):
                for f in range(4):
                    S0[f, k, c] = jnp.zeros((width, ny), jnp.float32)
                S0[4, k, c] = jnp.ones((width, ny), jnp.float32)

        @pl.when(jnp.logical_not(has_down))
        def _():
            outside_z(1)

        @pl.when(jnp.logical_not(has_up))
        def _():
            outside_z(1 + ZH + nl)

    def remote(src, dst, number, device):
        return pltpu.make_async_remote_copy(src_ref=src, dst_ref=dst, send_sem=send.at[number],
                                            recv_sem=recv.at[number], device_id=device, device_id_type=MESH)

    first, last = pl.ds(PAD, XH), pl.ds(PAD + nxl - XH, XH)
    from_left, from_right = pl.ds(PAD - XH, XH), pl.ds(PAD + nxl, XH)
    every = pl.ds(0, 5)
    leftward = [
        remote(S0.at[every, own, first], S0.at[every, own, from_right], 0, {"gx": left}),
        remote(G.at[:, first], G.at[:, from_right], 1, {"gx": left}),
        remote(M.at[first], M.at[from_right], 2, {"gx": left}),
    ]
    rightward = [
        remote(S0.at[every, own, last], S0.at[every, own, from_left], 3, {"gx": right}),
        remote(G.at[:, last], G.at[:, from_left], 4, {"gx": right}),
        remote(M.at[last], M.at[from_left], 5, {"gx": right}),
    ]
    top, bottom = pl.ds(base + nl - ZH, ZH), pl.ds(base, ZH)
    from_down, from_up = pl.ds(base_up - ZH, ZH), pl.ds(base_down + nl, ZH)
    pieces = (pl.ds(PAD, nxl), from_left, from_right)
    upward = [remote(S0.at[every, top, piece], S0.at[every, from_down, piece], 6 + n, {"gz": up})
              for n, piece in enumerate(pieces)]
    downward = [remote(S0.at[every, bottom, piece], S0.at[every, from_up, piece], 9 + n, {"gz": down})
                for n, piece in enumerate(pieces)]

    for n in range(5):
        copies[n].wait()
    pl.semaphore_wait(barrier, nz - 1 + jnp.where(has_left, 1, 0) + jnp.where(has_right, 1, 0))

    @pl.when(has_left)
    def _():
        for copy in leftward:
            copy.start()

    @pl.when(has_right)
    def _():
        for copy in rightward:
            copy.start()

    @pl.when(has_up)
    def _():
        upward[0].start()

    @pl.when(has_down)
    def _():
        downward[0].start()

    copies[5].wait()
    copies[6].wait()
    total = jnp.zeros((nxl, ny), jnp.float32)
    for k in reversed(range(nl)):
        cell = DN[k]
        DN[k] = total + 0.5 * cell
        total = total + cell
    FS[2, mine] = total

    def dy(f):
        axis = f.ndim - 1
        lane = lax.broadcasted_iota(jnp.int32, f.shape, axis)
        return (jnp.where(lane < ny - 1, pltpu.roll(f, ny - 1, axis), 0.0)
                - jnp.where(lane > 0, pltpu.roll(f, 1, axis), 0.0))

    def inside(start, height):
        column = gx * nxl + lax.broadcasted_iota(jnp.int32, (height, ny), 0) + (start - PAD)
        return (column >= 0) & (column < nx * nxl)

    def plan(start, height):
        c = slice(start, start + height)
        A[0, c] = 0.5 * (FX[start + 1:start + height + 1] - FX[start - 1:start + height - 1])
        A[1, c] = 0.5 * dy(FX[c])
        A[2, c] = jnp.where(inside(start, height) & (M[c] > 0), 1.0, 0.0)
        A[3, c] = jnp.where(M[c] == 1, FRICTION, 0.0)

    def level_at(k, count):
        return gz * nl + k - base + lax.broadcasted_iota(jnp.int32, (count, 1, ny), 0)

    def stress(B, k, count, start, height):
        at = pl.ds(k, count)
        c = slice(start, start + height)
        m, p = slice(start - 1, start + height - 1), slice(start + 1, start + height + 1)
        above, below = pl.ds(k + 1, count), pl.ds(k - 1, count)
        xx, vx, wx = (B[f, at, p] - B[f, at, m] for f in range(3))
        uz, vz, zz = (B[f, above, c] - B[f, below, c] for f in range(3))
        uy, yy, wy = (dy(B[f, at, c]) for f in range(3))
        xy, xz, yz = uy + vx, uz + wx, vz + wy
        twice = xx * xx + yy * yy + zz * zz
        second = 0.0625 * (twice + twice + (xy * xy + xz * xz + yz * yz))
        third = jnp.log2(S0[4, at, c] * (second + REGULAR)) * (1.0 / 3.0)
        a = jnp.exp2(-third)
        V[0, at, c] = (2.0 * STEP) * jnp.exp2(third)
        V[1, at, c] = (0.25 * STEP) * a * (xx + yy + zz)
        h = 0.25 * a
        if height == 8:
            h = jnp.where(jnp.broadcast_to(inside(start, height)[None], h.shape), h, 0.0)
        if nz > 2:
            level = level_at(k, count)
            ok = jnp.where((level >= 0) & (level < levels_total), 1.0, 0.0)
            h = jnp.where(jnp.broadcast_to(ok, h.shape) > 0.0, h, 0.0)
        g = 0.5 * h
        T[0, at, c] = g * xz
        T[1, at, c] = g * yz
        T[2, at, c] = h * zz
        T[3, at, c] = h * xx
        T[4, at, c] = g * xy
        T[5, at, c] = h * yy

    def move(B, k, count, start, height):
        at = pl.ds(k, count)
        c = slice(start, start + height)
        m, p = slice(start - 1, start + height - 1), slice(start + 1, start + height + 1)
        above, below = pl.ds(k + 1, count), pl.ds(k - 1, count)
        level = level_at(k, count)
        drag = jnp.where(level == 0, 1.0, 0.0) * A[3, c][None]
        u, v, press = B[0, at, c], B[1, at, c], B[3, at, c]
        fx = ((T[3, at, p] - T[3, at, m]) + dy(T[4, at, c]) + (T[0, above, c] - T[0, below, c])
              - 0.5 * (B[3, at, p] - B[3, at, m]) - A[0, c][None] - drag * u)
        fy = ((T[4, at, p] - T[4, at, m]) + dy(T[5, at, c]) + (T[1, above, c] - T[1, below, c])
              - 0.5 * dy(press) - A[1, c][None] - drag * v)
        fz = ((T[0, at, p] - T[0, at, m]) + dy(T[1, at, c]) + (T[2, above, c] - T[2, below, c])
              - 0.5 * (B[3, above, c] - B[3, below, c]))
        step = V[0, at, c]
        ice = jnp.broadcast_to(A[2, c][None], u.shape)
        if nz > 2:
            ice = ice * jnp.where((level >= 0) & (level < levels_total), 1.0, 0.0)
        return [jnp.where(ice > 0.0, value, 0.0) for value in (
            u + step * fx, v + step * fy, B[2, at, c] + step * fz, press - V[1, at, c])]

    def blocks(reach, most, step, areas):
        start, count = span(reach)
        pieces = -(-count // most)
        for n in range(pieces):
            one, two = count * n // pieces, count * (n + 1) // pieces
            for area in areas:
                step(start + one, two - one, *area)

    def stress_first(*at):
        stress(S0, *at)

    def stress_last(*at):
        stress(S1, *at)

    def move_first(k, count, start, height):
        for f, value in enumerate(move(S0, k, count, start, height)):
            S1[f, pl.ds(k, count), start:start + height] = value

    def move_last(k, count, start, height):
        for f, value in enumerate(move(S1, k, count, start, height)):
            flow_out[f, pl.ds(k - base, count), start:start + height] = value

    middle = [(PAD + 1, nxl - 2)]
    FX[mine] = G[1, mine] + G[0, mine]
    plan(*middle[0])
    for flag, group in ((has_down, upward), (has_up, downward)):
        @pl.when(flag)
        def _():
            group[0].wait_recv()

    blocks(3, 2, stress_first, middle)
    blocks(2, 2, move_first, middle)
    blocks(1, 2, stress_last, middle)

    @pl.when(has_left)
    def _():
        for copy in rightward:
            copy.wait_recv()

    @pl.when(has_left & has_up)
    def _():
        upward[1].start()

    @pl.when(has_left & has_down)
    def _():
        downward[1].start()

    @pl.when(has_right)
    def _():
        for copy in leftward:
            copy.wait_recv()

    @pl.when(has_right & has_up)
    def _():
        upward[2].start()

    @pl.when(has_right & has_down)
    def _():
        downward[2].start()

    blocks(0, 2, move_last, middle)

    ends = [(PAD - 4, 8), (PAD + nxl - 4, 8)]
    for start in (PAD - 8, PAD + nxl):
        strip = slice(start, start + 8)
        FX[strip] = G[1, strip] + G[0, strip]
    for area in ends:
        plan(*area)
    for flag, group in ((has_down, upward), (has_up, downward)):
        @pl.when(flag & has_left)
        def _():
            group[1].wait_recv()

        @pl.when(flag & has_right)
        def _():
            group[2].wait_recv()

    blocks(3, 6, stress_first, ends)
    blocks(2, 6, move_first, [(PAD - 5, 8), (PAD + nxl - 3, 8)])
    blocks(1, 6, stress_last, ends)
    blocks(0, 4, move_last, ends)
    sum_u, sum_v = flow_out[0, 0, c], flow_out[1, 0, c]
    for k in range(1, nl):
        sum_u = sum_u + flow_out[0, k, c]
        sum_v = sum_v + flow_out[1, k, c]
    FS[0, c] = sum_u
    FS[1, c] = sum_v

    sums = [pltpu.make_async_remote_copy(
        src_ref=FS.at[:, pl.ds(lo, width)], dst_ref=FR.at[off - 1, :, pl.ds(lo, width)],
        send_sem=fsend.at[off - 1], recv_sem=frecv.at[off - 1],
        device_id={"gz": lax.rem(gz + off, nz)}, device_id_type=MESH) for off in range(1, nz)]
    for copy in sums:
        copy.start()
    above = jnp.zeros((nxl, ny), jnp.float32)
    for off in range(1, nz):
        sums[off - 1].wait_recv()
        sum_u = sum_u + FR[off - 1, 0, c]
        sum_v = sum_v + FR[off - 1, 1, c]
        above = above + jnp.where(gz < off, 1.0, 0.0) * FR[off - 1, 2, mine]
    part = G[0, c] * (1.0 / levels_total)
    FX[c] = part * sum_u
    flux_y = dy(part * sum_v)[8:8 + nxl]
    spread = FX[PAD + 1:PAD + nxl + 1] - FX[PAD - 1:PAD + nxl - 1] + flux_y
    fresh = G[0, mine] + TIME_STEP * (SM[...] - 0.5 * spread)
    new_thickness[...] = fresh
    weight = fresh * (1.0 / levels_total)
    for k in range(nl):
        overburden[k] = weight * (above + DN[k])

    @pl.when(has_left)
    def _():
        for copy in leftward:
            copy.wait_send()

    @pl.when(has_right)
    def _():
        for copy in rightward:
            copy.wait_send()

    for flag, group in ((has_up, upward), (has_down, downward)):
        @pl.when(flag)
        def _():
            group[0].wait_send()

        @pl.when(flag & has_left)
        def _():
            group[1].wait_send()

        @pl.when(flag & has_right)
        def _():
            group[2].wait_send()

    for copy in sums:
        copy.wait_send()


def paired(nx, nl, nxl, flow, fluid, density, thickness, bed, smb, mask,
           flow_out, new_thickness, overburden,
           S0, S1, T, V, G, M, PK, RK, SM, DN, A, FX, FM, RM, FE, RE, FD, RD,
           loc, send, recv):
    gx, gz = lax.axis_index("gx"), lax.axis_index("gz")
    left, right = lax.rem(gx + nx - 1, nx), lax.rem(gx + 1, nx)
    has_left, has_right = gx > 0, gx < nx - 1
    odd = lax.rem(gx, 2)
    near = gx + 1 - 2 * odd
    far = lax.rem(gx + nx - 1 + 2 * odd, nx)
    has_far = jnp.where(odd == 1, gx, nx - 1 - gx) < nx - 1
    ny = flow.shape[-1]
    levels_total = 2 * nl
    depth, rows = S0.shape[1], S0.shape[2]
    base = 1 + ZH * gz
    own = pl.ds(base, nl)
    facing = pl.ds(1 + nl - ZH + gz * (2 * ZH - nl), ZH)
    others = pl.ds(1 + gz * 2 * ZH, nl - ZH)
    across = pl.ds(1 + gz * nl, ZH)
    mine = slice(PAD, PAD + nxl)

    barrier = pltpu.get_barrier_semaphore()
    pl.semaphore_signal(barrier, inc=1, device_id={"gx": near}, device_id_type=MESH)
    pl.semaphore_signal(barrier, inc=1, device_id={"gz": 1 - gz}, device_id_type=MESH)

    @pl.when(has_far)
    def _():
        pl.semaphore_signal(barrier, inc=1, device_id={"gx": far}, device_id_type=MESH)

    copies = [
        pltpu.make_async_copy(flow, S0.at[pl.ds(0, 4), own, mine], loc.at[0]),
        pltpu.make_async_copy(fluid, S0.at[4, own, mine], loc.at[1]),
        pltpu.make_async_copy(thickness, G.at[0, mine], loc.at[2]),
        pltpu.make_async_copy(bed, G.at[1, mine], loc.at[3]),
        pltpu.make_async_copy(mask, M, loc.at[4]),
        pltpu.make_async_copy(density, DN, loc.at[5]),
        pltpu.make_async_copy(smb, SM, loc.at[6]),
    ]
    for copy in copies:
        copy.start()

    zrow = jnp.zeros((rows, ny), jnp.float32)
    for k in (0, depth - 1):
        for f in range(4):
            S0[f, k] = zrow
            S1[f, k] = zrow
        for f in range(3):
            T[f, k] = zrow

    def outside_x(where):
        strip = slice(PAD - 8, PAD) if where == 0 else slice(PAD + nxl, PAD + nxl + 8)
        zero = jnp.zeros((8, ny), jnp.float32)

        def one(k, _):
            for f in range(4):
                S0[f, k, strip] = zero
            S0[4, k, strip] = zero + 1.0
            return 0

        lax.fori_loop(1, depth - 1, one, 0)
        G[0, strip] = zero
        G[2, strip] = zero
        FX[strip] = zero

    @pl.when(jnp.logical_not(has_left))
    def _():
        outside_x(0)

    @pl.when(jnp.logical_not(has_right))
    def _():
        outside_x(1)

    def remote(src, dst, number, device):
        return pltpu.make_async_remote_copy(src_ref=src, dst_ref=dst, send_sem=send.at[number],
                                            recv_sem=recv.at[number], device_id=device, device_id_type=MESH)

    motion, state = pl.ds(0, 3), pl.ds(3, 2)

    def halo(levels, src, dst, number, device):
        (src_uvw, src_pf), (dst_uvw, dst_pf) = src, dst
        return [remote(S0.at[motion, levels, src_uvw], S0.at[motion, levels, dst_uvw], number, device),
                remote(S0.at[state, levels, src_pf], S0.at[state, levels, dst_pf], number + 1, device)]

    first = pl.ds(PAD, XH), pl.ds(PAD, XH - 1)
    last = pl.ds(PAD + nxl - XH, XH), pl.ds(PAD + nxl - XH + 1, XH - 1)
    from_left = pl.ds(PAD - XH, XH), pl.ds(PAD - XH + 1, XH - 1)
    from_right = pl.ds(PAD + nxl, XH), pl.ds(PAD + nxl, XH - 1)

    def sideways(src, dst, side, number, device):
        early = halo(facing, src, dst, number, device)
        early.append(remote(PK.at[side], RK.at[1 - side], number + 2, device))
        return early, halo(others, src, dst, number + 3, device)

    leftward = sideways(first, from_right, 0, 0, {"gx": left})
    rightward = sideways(last, from_left, 1, 5, {"gx": right})
    partner = {"gz": 1 - gz}
    planes = remote(S0.at[pl.ds(0, 5), facing, pl.ds(PAD, nxl)], S0.at[pl.ds(0, 5), across, pl.ds(PAD, nxl)], 10, partner)

    def corner(at, number):
        (uvw, pf) = at
        return [remote(S0.at[motion, facing, uvw], S0.at[motion, across, uvw], number, partner),
                remote(S0.at[state, facing, pf], S0.at[state, across, pf], number + 1, partner)]

    corners = corner(from_left, 11), corner(from_right, 13)
    weights = remote(FD, RD, 15, partner)
    inner = remote(FM, RM, 16, partner)
    strips = [remote(FE.at[side], RE.at[side], 17 + side, partner) for side in range(2)]
    incoming = rightward, leftward
    have = (has_left, has_right)

    for n in range(5):
        copies[n].wait()
    G[2, mine] = M[...].astype(jnp.float32)
    FX[mine] = G[1, mine] + G[0, mine]
    end = PAD + nxl
    PK[0, 0:4] = FX[PAD:PAD + 4]
    PK[0, 4:7] = G[2, PAD:PAD + 3]
    PK[0, 7:8] = G[0, PAD:PAD + 1]
    PK[1, 0:4] = FX[end - 4:end]
    PK[1, 4:7] = G[2, end - 3:end]
    PK[1, 7:8] = G[0, end - 1:end]

    pl.semaphore_wait(barrier, 2 + jnp.where(has_far, 1, 0))

    def launch(group, flag):
        @pl.when(flag)
        def _():
            for copy in group:
                copy.start()

    launch(leftward[0], odd == 1)
    launch(rightward[0], odd == 0)
    eager = lax.rem(gx + 1, 4) < 2
    launch(leftward[1], (odd == 1) & eager)
    launch(rightward[1], (odd == 0) & eager)
    planes.start()

    launch(rightward[0], (odd == 1) & has_right)
    launch(leftward[0], (odd == 0) & has_left & jnp.logical_not(eager))
    launch(leftward[1], (odd == 1) & jnp.logical_not(eager))
    launch(rightward[1], (odd == 0) & jnp.logical_not(eager))
    launch(rightward[1], (odd == 1) & has_right)
    launch(leftward[1], (odd == 0) & has_left & jnp.logical_not(eager))


    def dy(f):
        axis = f.ndim - 1
        lane = lax.broadcasted_iota(jnp.int32, f.shape, axis)
        return (jnp.where(lane < ny - 1, pltpu.roll(f, ny - 1, axis), 0.0)
                - jnp.where(lane > 0, pltpu.roll(f, 1, axis), 0.0))

    def inside(start, height):
        column = gx * nxl + lax.broadcasted_iota(jnp.int32, (height, ny), 0) + (start - PAD)
        return (column >= 0) & (column < nx * nxl)

    def plan(start, height):
        c = slice(start, start + height)
        A[0, c] = 0.5 * (FX[start + 1:start + height + 1] - FX[start - 1:start + height - 1])
        A[1, c] = 0.5 * dy(FX[c])
        A[2, c] = jnp.where(inside(start, height) & (G[2, c] > 0.0), 1.0, 0.0)
        A[3, c] = jnp.where(G[2, c] == 1.0, FRICTION, 0.0)

    def level_at(k, count):
        return gz * nl + k - base + lax.broadcasted_iota(jnp.int32, (count, 1, ny), 0)

    def stress(B, k, count, start, height):
        at = pl.ds(k, count)
        c = slice(start, start + height)
        m, p = slice(start - 1, start + height - 1), slice(start + 1, start + height + 1)
        above, below = pl.ds(k + 1, count), pl.ds(k - 1, count)
        xx, vx, wx = (B[f, at, p] - B[f, at, m] for f in range(3))
        uz, vz, zz = (B[f, above, c] - B[f, below, c] for f in range(3))
        uy, yy, wy = (dy(B[f, at, c]) for f in range(3))
        xy, xz, yz = uy + vx, uz + wx, vz + wy
        twice = xx * xx + yy * yy + zz * zz
        second = 0.0625 * (twice + twice + (xy * xy + xz * xz + yz * yz))
        third = jnp.log2(S0[4, at, c] * (second + REGULAR)) * (1.0 / 3.0)
        a = jnp.exp2(-third)
        V[0, at, c] = (2.0 * STEP) * jnp.exp2(third)
        V[1, at, c] = (0.25 * STEP) * a * (xx + yy + zz)
        h = 0.25 * a
        if height == 8:
            h = jnp.where(jnp.broadcast_to(inside(start, height)[None], h.shape), h, 0.0)
        g = 0.5 * h
        q = 0.5 * B[3, at, c]
        T[0, at, c] = g * xz
        T[1, at, c] = g * yz
        T[2, at, c] = h * zz - q
        T[3, at, c] = h * xx - q
        T[4, at, c] = g * xy
        T[5, at, c] = h * yy - q

    def move(B, k, count, start, height):
        at = pl.ds(k, count)
        c = slice(start, start + height)
        m, p = slice(start - 1, start + height - 1), slice(start + 1, start + height + 1)
        above, below = pl.ds(k + 1, count), pl.ds(k - 1, count)
        drag = jnp.where(level_at(k, count) == 0, 1.0, 0.0) * A[3, c][None]
        u, v, press = B[0, at, c], B[1, at, c], B[3, at, c]
        fx = ((T[3, at, p] - T[3, at, m]) + dy(T[4, at, c]) + (T[0, above, c] - T[0, below, c])
              - A[0, c][None] - drag * u)
        fy = ((T[4, at, p] - T[4, at, m]) + dy(T[5, at, c]) + (T[1, above, c] - T[1, below, c])
              - A[1, c][None] - drag * v)
        fz = ((T[0, at, p] - T[0, at, m]) + dy(T[1, at, c]) + (T[2, above, c] - T[2, below, c]))
        step = V[0, at, c]
        ice = jnp.broadcast_to(A[2, c][None], u.shape)
        return [jnp.where(ice > 0.0, value, 0.0) for value in (
            u + step * fx, v + step * fy, B[2, at, c] + step * fz, press - V[1, at, c])]

    def blocks(start, count, most, step, area):
        pieces = -(-count // most)
        for n in range(pieces):
            one, two = count * n // pieces, count * (n + 1) // pieces
            step(start + one, two - one, *area)

    def apart(reach, most, step, area):
        blocks(1 + gz * (2 * ZH - reach), nl - ZH + reach, most, step, area)

    def facing_part(reach, most, step, area):
        low, high = 1 + nl - ZH + reach, 1 + ZH - reach
        blocks(low + gz * (high - low), ZH, most, step, area)

    def reached(reach, most, step, area):
        low = 1 + nl - reach
        blocks(low + gz * (1 + ZH - reach - low), 2 * (ZH - 4 + reach), most, step, area)

    def rest(reach, most, step, area):
        count = nl - reach
        blocks(1 + gz * (ZH + nl - count), count, most, step, area)

    def stress_first(*at):
        stress(S0, *at)

    def stress_last(*at):
        stress(S1, *at)

    def move_first(k, count, start, height):
        for f, value in enumerate(move(S0, k, count, start, height)):
            S1[f, pl.ds(k, count), start:start + height] = value

    def move_last(k, count, start, height):
        for f, value in enumerate(move(S1, k, count, start, height)):
            flow_out[f, pl.ds(k - base, count), start:start + height] = value

    middle = (PAD + 1, nxl - 2)
    plan(*middle)
    apart(3, 2, stress_first, middle)

    copies[5].wait()
    copies[6].wait()
    total = jnp.zeros((nxl, ny), jnp.float32)
    for k in reversed(range(nl)):
        cell = DN[k]
        DN[k] = total + 0.5 * cell
        total = total + cell
    FD[...] = total
    weights.start()

    apart(2, 2, move_first, middle)
    apart(1, 2, stress_last, middle)
    launch(leftward[0], (odd == 0) & has_left & eager)
    launch(leftward[1], (odd == 0) & has_left & eager)
    apart(0, 2, move_last, middle)
    planes.wait_recv()
    facing_part(3, 2, stress_first, middle)

    def forward(side):
        @pl.when(have[side])
        def _():
            for copy in incoming[side][0][:2]:
                copy.wait_recv()
            for copy in corners[side]:
                copy.start()

    left_leads = (gx == 0) | ((odd == 1) & has_right)

    def by_arrival(step):
        @pl.when(left_leads)
        def _():
            step(0, 1)

        @pl.when(jnp.logical_not(left_leads))
        def _():
            step(1, 0)

    facing_part(2, 2, move_first, middle)
    facing_part(1, 2, stress_last, middle)
    facing_part(0, 2, move_last, middle)

    by_arrival(lambda lead, other: forward(lead))

    def depth_sum(f, c):
        value = flow_out[f, 0, c]
        for k in range(1, nl):
            value = value + flow_out[f, k, c]
        return value

    for f in range(2):
        FM[f] = depth_sum(f, mine)
    inner.start()

    edges = [((PAD - 4, 8), (PAD - 5, 8)), ((PAD + nxl - 4, 8), (PAD + nxl - 3, 8))]

    def approach(side):
        area, shifted = edges[side]

        @pl.when(have[side])
        def _():
            incoming[side][0][2].wait_recv()
            at = PAD if side == 0 else end
            for row in range(4):
                to = at - 4 + row if side == 0 else at + row
                FX[to:to + 1] = RK[side, row:row + 1]
            for row in range(3):
                to = at - 3 + row if side == 0 else at + row
                G[2, to:to + 1] = RK[side, 4 + row:5 + row]
            to = at - 1 if side == 0 else at
            G[0, to:to + 1] = RK[side, 7:8]
            for copy in corners[side]:
                copy.wait_recv()

        plan(*area)
        reached(3, 3, stress_first, area)
        reached(2, 4, move_first, shifted)
        reached(1, 4, stress_last, area)

    def finish(side):
        area, shifted = edges[side]

        @pl.when(have[side])
        def _():
            for copy in incoming[side][1]:
                copy.wait_recv()

        rest(3, 3, stress_first, area)
        rest(2, 3, move_first, shifted)
        rest(1, 4, stress_last, area)
        rest(0, 4, move_last, area)
        wide = slice(PAD - 8, PAD + 8) if side == 0 else slice(PAD + nxl - 8, PAD + nxl + 8)
        for f in range(2):
            FE[side, f] = depth_sum(f, wide)
        strips[side].start()

    def both(lead, other):
        forward(other)
        approach(lead)
        finish(lead)
        approach(other)
        finish(other)

    by_arrival(both)

    def settle(start, height, sum_v):
        c = slice(start, start + height)
        o = slice(start - PAD, start - PAD + height)
        flux_y = dy(G[0, c] * (1.0 / levels_total) * sum_v)
        spread = FX[start + 1:start + height + 1] - FX[start - 1:start + height - 1] + flux_y
        fresh = G[0, c] + TIME_STEP * (SM[o] - 0.5 * spread)
        new_thickness[o] = fresh
        weight = fresh * (1.0 / levels_total)
        above = jnp.where(gz == 0, 1.0, 0.0) * RD[o]
        for k in range(nl):
            overburden[k, o] = weight * (above + DN[k, o])

    weights.wait_recv()
    inner.wait_recv()
    FX[mine] = G[0, mine] * (1.0 / levels_total) * (FM[0] + RM[0])
    settle(PAD + 8, nxl - 16, FM[1, 8:nxl - 8] + RM[1, 8:nxl - 8])
    def conclude(side):
        strips[side].wait_recv()
        begin = PAD - 8 if side == 0 else PAD + nxl - 8
        wide = slice(begin, begin + 16)
        FX[wide] = G[0, wide] * (1.0 / levels_total) * (FE[side, 0] + RE[side, 0])
        inward = slice(8, 16) if side == 0 else slice(0, 8)
        settle(PAD if side == 0 else PAD + nxl - 8, 8, FE[side, 1, inward] + RE[side, 1, inward])

    def close(lead, other):
        conclude(lead)
        conclude(other)

    by_arrival(close)

    for side, group in ((0, leftward), (1, rightward)):
        @pl.when(have[side])
        def _():
            for copy in (*group[0], *group[1], *corners[side]):
                copy.wait_send()

    for copy in (planes, weights, inner, *strips):
        copy.wait_send()


def write(nxl, held, fresh, weight, flow_out, new_thickness, overburden, done):
    copies = [
        pltpu.make_async_copy(held.at[:, :, pl.ds(PAD, nxl)], flow_out, done.at[0]),
        pltpu.make_async_copy(fresh, new_thickness, done.at[1]),
        pltpu.make_async_copy(weight, overburden, done.at[2]),
    ]
    for copy in copies:
        copy.start()
    for copy in copies:
        copy.wait()


def solution(mesh):
    nx, nz = mesh.shape["gx"], mesh.shape["gz"]

    def body(flow, fluid, density, thickness, bed, smb, mask):
        nl, nxl, ny = fluid.shape
        depth = nl + 2 + (ZH if nz == 2 else 2 * ZH)
        rows = nxl + 2 * PAD
        f32 = jnp.float32
        vmem = pl.BlockSpec(memory_space=pltpu.VMEM)
        block = [pltpu.VMEM((n, depth, rows, ny), f32) for n in (5, 4, 6, 2)]
        if nz == 2 and nx % 2 == 0 and nl > ZH and nxl >= 24:
            body_of = functools.partial(paired, nx, nl, nxl)
            scratch = block + [
                pltpu.VMEM((3, rows, ny), f32),
                pltpu.VMEM((nxl, ny), jnp.int32),
                pltpu.VMEM((2, 8, ny), f32),
                pltpu.VMEM((2, 8, ny), f32),
                pltpu.VMEM((nxl, ny), f32),
                pltpu.VMEM((nl, nxl, ny), f32),
                pltpu.VMEM((4, rows, ny), f32),
                pltpu.VMEM((rows, ny), f32),
                pltpu.VMEM((2, nxl, ny), f32),
                pltpu.VMEM((2, nxl, ny), f32),
                pltpu.VMEM((2, 2, 16, ny), f32),
                pltpu.VMEM((2, 2, 16, ny), f32),
                pltpu.VMEM((nxl, ny), f32),
                pltpu.VMEM((nxl, ny), f32),
                pltpu.SemaphoreType.DMA((7,)),
                pltpu.SemaphoreType.DMA((19,)),
                pltpu.SemaphoreType.DMA((19,)),
            ]
        else:
            body_of = functools.partial(kernel, nx, nz, nl, nxl)
            scratch = block + [
                pltpu.VMEM((2, rows, ny), f32),
                pltpu.VMEM((rows, ny), jnp.int32),
                pltpu.VMEM((nxl, ny), f32),
                pltpu.VMEM((nl, nxl, ny), f32),
                pltpu.VMEM((4, rows, ny), f32),
                pltpu.VMEM((rows, ny), f32),
                pltpu.VMEM((3, rows, ny), f32),
                pltpu.VMEM((nz - 1, 3, rows, ny), f32),
                pltpu.SemaphoreType.DMA((7,)),
                pltpu.SemaphoreType.DMA((12,)),
                pltpu.SemaphoreType.DMA((12,)),
                pltpu.SemaphoreType.DMA((nz - 1,)),
                pltpu.SemaphoreType.DMA((nz - 1,)),
            ]
        held, fresh, weight = pl.pallas_call(
            body_of,
            out_shape=(
                pltpu.VMEM((4, nl, rows, ny), f32),
                pltpu.VMEM(thickness.shape, f32),
                pltpu.VMEM(density.shape, f32),
            ),
            in_specs=[pl.BlockSpec(memory_space=pl.ANY)] * 7,
            out_specs=(vmem, vmem, vmem),
            scratch_shapes=scratch,
            compiler_params=pltpu.CompilerParams(collective_id=0, has_side_effects=True),
        )(flow, fluid, density, thickness, bed, smb, mask)
        anywhere = pl.BlockSpec(memory_space=pl.ANY)
        return pl.pallas_call(
            functools.partial(write, nxl),
            out_shape=(
                jax.ShapeDtypeStruct(flow.shape, f32),
                jax.ShapeDtypeStruct(thickness.shape, f32),
                jax.ShapeDtypeStruct(density.shape, f32),
            ),
            in_specs=[vmem] * 3,
            out_specs=(anywhere,) * 3,
            scratch_shapes=[pltpu.SemaphoreType.DMA((3,))],
        )(*(pltpu.with_memory_space_constraint(x, pltpu.VMEM) for x in (held, fresh, weight)))

    placed = (
        P(None, "gz", "gx", None), P("gz", "gx", None), P("gz", "gx", None),
        P("gx", None), P("gx", None), P("gx", None), P("gx", None),
    )
    return jax.shard_map(
        body, mesh=mesh, in_specs=placed,
        out_specs=(P(None, "gz", "gx", None), P("gx", None), P("gz", "gx", None)),
        check_vma=False,
    )
```
